32 devices in a mesh: dp: 16 (over z, y, core), tensor: 2 (over x).
Axes of the slice: x: 2, y: 2, z: 4, core: 2. Of those that a mesh axis runs over, the one named last changes fastest.
Arguments:
- tokens: bfloat16 [8192, 2048], P(('dp', 'tensor')), may hold values from -6 to 6
- cotangent: bfloat16 [8192, 2048], P(('dp', 'tensor')), may hold values from -6 to 6
- norm_gain: bfloat16 [2048], replicated, may hold values from 0.099609375 to 1.8984375
- w_gate: bfloat16 [2048, 4096], P('dp', 'tensor'), may hold values from -0.125 to 0.125
- w_input: bfloat16 [2048, 4096], P('dp', 'tensor'), may hold values from -0.125 to 0.125
- w_state: bfloat16 [2048, 256], P('dp'), may hold values from -0.125 to 0.125
- w_step: bfloat16 [2048, 64], P('dp', 'tensor'), may hold values from -0.125 to 0.125
- conv_weight: bfloat16 [4, 4096], P(None, 'tensor'), may hold values from -3 to 3
- conv_bias: bfloat16 [4096], P('tensor'), may hold values from -3 to 3
- conv_state_weight: bfloat16 [4, 256], replicated, may hold values from -3 to 3
- conv_state_bias: bfloat16 [256], replicated, may hold values from -3 to 3
- step_bias: bfloat16 [64], P('tensor'), may hold values from -6.875 to -2.25
- decay_log: bfloat16 [64], P('tensor'), may hold values from 0 to 2.765625
- skip_gain: bfloat16 [64], P('tensor'), may hold values from -1 to 1
- gate_gain: bfloat16 [4096], P('tensor'), may hold values from 0.099609375 to 1.8984375
- w_out: bfloat16 [2048, 4096], P('dp', 'tensor'), may hold values from -0.09375 to 0.09375
- stats_gate: float32 [32, 64, 2, 64, 64], P('dp', 'tensor'), as said below
- stats_input: float32 [32, 64, 2, 64, 64], P('dp', 'tensor'), as said below
- stats_state: float32 [32, 4, 2, 64, 64], P('dp'), as said below
- stats_out: float32 [32, 64, 2, 64, 64], P('dp', 'tensor'), as said below
- roots_gate: float32 [32, 64, 2, 64, 64], P('dp', 'tensor'), as said below
- roots_input: float32 [32, 64, 2, 64, 64], P('dp', 'tensor'), as said below
- roots_state: float32 [32, 4, 2, 64, 64], P('dp'), as said below
- roots_out: float32 [32, 64, 2, 64, 64], P('dp', 'tensor'), as said below
- seq_lens: int32 [16, 4], P('dp'), may hold values from 1 to 384, 512 in all within a row
- balance_perm: int32 [8192], P('dp'), may hold values from 0 to 8191, as said below
- inverse_perm: int32 [8192], P(('dp', 'tensor')), may hold values from 0 to 8191, as said below
Outputs:
- block_out: float32 [8192, 2048], P(('dp', 'tensor'))
- tokens_grad: float32 [8192, 2048], P(('dp', 'tensor'))
- norm_gain_grad: float32 [2048], replicated
- w_gate_grad: float32 [2048, 4096], P('dp', 'tensor')
- w_input_grad: float32 [2048, 4096], P('dp', 'tensor')
- w_state_grad: float32 [2048, 256], P('dp')
- w_step_grad: float32 [2048, 64], P('dp', 'tensor')
- conv_weight_grad: float32 [4, 4096], P(None, 'tensor')
- conv_bias_grad: float32 [4096], P('tensor')
- conv_state_weight_grad: float32 [4, 256], replicated
- conv_state_bias_grad: float32 [256], replicated
- step_bias_grad: float32 [64], P('tensor')
- decay_log_grad: float32 [64], P('tensor')
- skip_gain_grad: float32 [64], P('tensor')
- gate_gain_grad: float32 [4096], P('tensor')
- w_out_grad: float32 [2048, 4096], P('dp', 'tensor')
- stats_gate_new: float32 [32, 64, 2, 64, 64], P('dp', 'tensor')
- stats_input_new: float32 [32, 64, 2, 64, 64], P('dp', 'tensor')
- stats_state_new: float32 [32, 4, 2, 64, 64], P('dp')
- stats_out_new: float32 [32, 64, 2, 64, 64], P('dp', 'tensor')
- master_gate: float32 [2048, 4096], P('dp', 'tensor')
- master_input: float32 [2048, 4096], P('dp', 'tensor')
- master_state: float32 [2048, 256], P('dp')
- master_out: float32 [2048, 4096], P('dp', 'tensor')
- copy_gate: bfloat16 [2048, 4096], P('dp', 'tensor')
- copy_input: bfloat16 [2048, 4096], P('dp', 'tensor')
- copy_state: bfloat16 [2048, 256], P('dp')
- copy_out: bfloat16 [2048, 4096], P('dp', 'tensor')
The draws below stay inside these ranges and needn't reach their ends.
Inputs may be any that keep to these rules, and one draw needn't show every extreme that they name: `seq_lens`: row g lists the lengths of the 4 sequences that fill balanced positions g * 512 to (g + 1) * 512 - 1 one after another. balance_perm is a permutation; of the 256 given positions d * 256 to (d + 1) * 256 - 1 of each device d, exactly 16 land in the 512 balanced positions of each group. `inverse_perm`: the inverse permutation of balance_perm. `stats_gate`: both matrices of each block pair are symmetric. `stats_input`: both matrices of each block pair are symmetric. `stats_state`: both matrices of each block pair are symmetric. `stats_out`: both matrices of each block pair are symmetric. `roots_gate`: both matrices of each block pair are symmetric. `roots_input`: both matrices of each block pair are symmetric. `roots_state`: both matrices of each block pair are symmetric. `roots_out`: both matrices of each block pair are symmetric.
All inputs are finite; a program needn't handle non-finite values.
Results may differ from the reference program's by a relative error of at most 0.019.
Values may be sent and summed in bfloat16 or wider, within the bound.
A program may use at most 256 MiB of HBM per device.

```python
import math
import jax
import jax.numpy as jnp
import numpy as np
from jax import lax

D = 2048
HEADS = 64
STATE = 128
KCONV = 4
SPAN = 256
BLK = 64
SEQ_GRP = 4
TOK_DEV = 256
INNER = 4096
TOK_GRP = 512
TOKENS = 8192
SLOT = 16
LONGEST = 384
N_DP = 16
N_TENSOR = 2


def balanced_order(key):
    key_slots, key_rows = jax.random.split(jax.random.fold_in(key, 11))
    slots = jax.vmap(lambda sub_key: jax.random.permutation(sub_key, TOK_GRP))(jax.random.split(key_slots, N_DP)).astype(jnp.int32)
    row_orders = jax.vmap(lambda sub_key: jax.random.permutation(sub_key, TOK_DEV))(jax.random.split(key_rows, N_DP * N_TENSOR)).astype(jnp.int32)
    source = slots // SLOT
    within_slot = slots % SLOT
    group_index = jnp.arange(N_DP, dtype=jnp.int32)[:, None]
    picked = row_orders[source, group_index * SLOT + within_slot]
    forward_map = (source * TOK_DEV + picked).reshape(TOKENS).astype(jnp.int32)
    backward_map = jnp.zeros((TOKENS,), jnp.int32).at[forward_map].set(jnp.arange(TOKENS, dtype=jnp.int32))
    return (forward_map, backward_map)


def draw_balance_perm(key, part):
    return balanced_order(key)[0]


def draw_inverse_perm(key, part):
    return balanced_order(key)[1]


def grad_level():
    return 0.5 * math.sqrt(TOKENS)


def stat_level():
    return grad_level() ** 2 * math.sqrt(BLK) / 4.0


def root_level():
    return (math.sqrt(D) * grad_level() * 3.2 * BLK) ** (-0.5)


def spd_blocks(key, block_shape, level_scale):
    key_off, key_diag = jax.random.split(key)
    noise_part = jax.random.normal(key_off, block_shape, jnp.float32) * level_scale
    symmetric = 0.5 * (noise_part + jnp.swapaxes(noise_part, -1, -2))
    diagonal = jax.random.uniform(key_diag, block_shape[:-1], jnp.float32, 2.0, 6.0) * level_scale * math.sqrt(block_shape[-1])
    return symmetric + diagonal[..., None] * jnp.eye(block_shape[-1], dtype=jnp.float32)


def draw_stats_gate(key, part):
    return spd_blocks(jax.random.fold_in(key, 1), (D // BLK, INNER // BLK, 2, BLK, BLK), stat_level())


def draw_stats_input(key, part):
    return spd_blocks(jax.random.fold_in(key, 2), (D // BLK, INNER // BLK, 2, BLK, BLK), stat_level())


def draw_stats_state(key, part):
    return spd_blocks(jax.random.fold_in(key, 3), (D // BLK, 2 * STATE // BLK, 2, BLK, BLK), stat_level())


def draw_stats_out(key, part):
    return spd_blocks(jax.random.fold_in(key, 4), (D // BLK, INNER // BLK, 2, BLK, BLK), stat_level())


def draw_roots_gate(key, part):
    return spd_blocks(jax.random.fold_in(key, 5), (D // BLK, INNER // BLK, 2, BLK, BLK), root_level())


def draw_roots_input(key, part):
    return spd_blocks(jax.random.fold_in(key, 6), (D // BLK, INNER // BLK, 2, BLK, BLK), root_level())


def draw_roots_state(key, part):
    return spd_blocks(jax.random.fold_in(key, 7), (D // BLK, 2 * STATE // BLK, 2, BLK, BLK), root_level())


def draw_roots_out(key, part):
    return spd_blocks(jax.random.fold_in(key, 8), (D // BLK, INNER // BLK, 2, BLK, BLK), root_level())


def shard_levels(key, shape, shards, low, high):
    def one(axis_at, parts):
        draws = jax.random.uniform(jax.random.fold_in(jax.random.fold_in(key, 6), axis_at), (parts,), jnp.float32, low / len(shards), high / len(shards))
        return jnp.repeat(jnp.exp(draws), shape[axis_at] // parts).reshape((-1,) + (1,) * (len(shape) - axis_at - 1))

    level = one(*shards[0])
    for cut in shards[1:]:
        level = level * one(*cut)
    return level


def split_up(count, total, bound, slope):
    loads = [(1 << 20) // math.isqrt(grade ** slope) + 1 for grade in range(2, count + 1)]
    spare, given = total - bound - (count - 1), [1] * (count - 1)
    while spare > 0:
        movable = [i for i in range(count - 1) if given[i] < bound]
        whole, remaining = sum([loads[i] for i in movable]), spare
        for i in movable:
            extra = min(bound - given[i], max(1, remaining * loads[i] // whole), spare)
            given[i] = given[i] + extra
            spare = spare - extra
    return np.array([bound] + given)


def uneven(key, count, total, bound, lean):
    if count == 2:
        one = jax.random.randint(key, (), max(1, total - bound), min(bound, total - 1) + 1)
        return jnp.stack([one, total - one])
    tallies = jnp.asarray(split_up(count, total, bound, lean), jnp.int32)
    twos = (count - 1) // 2
    donor, taker = tallies[1:1 + 2 * twos:2], tallies[2:2 + 2 * twos:2]
    margin = jnp.minimum(donor - 1, bound - taker)
    moved = jax.random.randint(jax.random.fold_in(key, 1), (twos,), 0, 1 << 20) % (margin + 1)
    tallies = tallies.at[1:1 + 2 * twos:2].set(donor - moved).at[2:2 + 2 * twos:2].set(taker + moved)
    return tallies[jax.random.permutation(jax.random.fold_in(key, 2), count)]


def scatter_about(rng, dims, scale, limit, shards=(), kind=jnp.bfloat16):
    gain = shard_levels(rng, dims, shards, -0.22, 0.18) if shards else 1.0
    result = jax.random.normal(rng, dims, jnp.float32) * scale * gain
    return jnp.minimum(jnp.maximum(result, -limit), limit).astype(kind)


def setup_inputs(seed: int = 0) -> dict:
    keys = jax.random.split(jax.random.key(seed), 28)
    tokens = scatter_about(keys[0], (TOKENS, D), 1.0, 6.0, ((0, 32),))
    cotangent = scatter_about(keys[1], (TOKENS, D), 1.0, 6.0, ((0, 32),))
    norm_gain = jnp.clip(1.0 + 0.18 * jax.random.normal(keys[2], (D,), jnp.float32), 0.099609375, 1.8984375).astype(jnp.bfloat16)
    w_gate = scatter_about(keys[3], (D, INNER), D ** -0.5, 0.125, ((0, 16), (1, 2)))
    w_input = scatter_about(keys[4], (D, INNER), D ** -0.5, 0.125, ((0, 16), (1, 2)))
    w_state = scatter_about(keys[5], (D, 2 * STATE), D ** -0.5, 0.125, ((0, 16),))
    w_step = scatter_about(keys[6], (D, HEADS), D ** -0.5, 0.125, ((0, 16), (1, 2)))
    conv_weight = scatter_about(keys[7], (KCONV, INNER), KCONV ** -0.5, 3.0, ((1, 2),))
    conv_bias = scatter_about(keys[8], (INNER,), 0.5, 3.0, ((0, 2),))
    conv_state_weight = scatter_about(keys[9], (KCONV, 2 * STATE), KCONV ** -0.5, 3.0)
    conv_state_bias = scatter_about(keys[10], (2 * STATE,), 0.5, 3.0)
    step_bias = jnp.clip(-6.875 + 4.625 * jax.random.uniform(keys[11], (HEADS,), jnp.float32) ** shard_levels(keys[11], (HEADS,), ((0, 2),), -0.2, 0.2), -6.875, -2.25).astype(jnp.bfloat16)
    decay_log = jnp.clip(2.765625 * jax.random.uniform(keys[12], (HEADS,), jnp.float32) ** shard_levels(keys[12], (HEADS,), ((0, 2),), -0.2, 0.2), 0.0, 2.765625).astype(jnp.bfloat16)
    skip_gain = jnp.clip(jax.random.uniform(keys[13], (HEADS,), jnp.float32, -1.0, 1.0) * shard_levels(keys[13], (HEADS,), ((0, 2),), -0.4, 0.0), -1.0, 1.0).astype(jnp.bfloat16)
    gate_gain = jnp.clip(1.0 + 0.18 * jax.random.normal(keys[14], (INNER,), jnp.float32), 0.099609375, 1.8984375).astype(jnp.bfloat16)
    w_out = scatter_about(keys[15], (D, INNER), INNER ** -0.5, 0.09375, ((0, 16), (1, 2)))
    stats_gate = draw_stats_gate(jax.random.fold_in(keys[27], 71), 0)
    stats_input = draw_stats_input(jax.random.fold_in(keys[27], 71), 0)
    stats_state = draw_stats_state(jax.random.fold_in(keys[27], 71), 0)
    stats_out = draw_stats_out(jax.random.fold_in(keys[27], 71), 0)
    roots_gate = draw_roots_gate(jax.random.fold_in(keys[27], 71), 0)
    roots_input = draw_roots_input(jax.random.fold_in(keys[27], 71), 0)
    roots_state = draw_roots_state(jax.random.fold_in(keys[27], 71), 0)
    roots_out = draw_roots_out(jax.random.fold_in(keys[27], 71), 0)
    seq_lens = jax.vmap(lambda own: uneven(own, SEQ_GRP, TOK_GRP, LONGEST, 2))(jax.random.split(keys[24], N_DP)).reshape((N_DP, SEQ_GRP)).astype(jnp.int32)
    balance_perm = draw_balance_perm(jax.random.fold_in(keys[27], 71), 0)
    inverse_perm = draw_inverse_perm(jax.random.fold_in(keys[27], 71), 0)
    return {"tokens": tokens, "cotangent": cotangent, "norm_gain": norm_gain, "w_gate": w_gate, "w_input": w_input, "w_state": w_state, "w_step": w_step, "conv_weight": conv_weight, "conv_bias": conv_bias, "conv_state_weight": conv_state_weight, "conv_state_bias": conv_state_bias, "step_bias": step_bias, "decay_log": decay_log, "skip_gain": skip_gain, "gate_gain": gate_gain, "w_out": w_out, "stats_gate": stats_gate, "stats_input": stats_input, "stats_state": stats_state, "stats_out": stats_out, "roots_gate": roots_gate, "roots_input": roots_input, "roots_state": roots_state, "roots_out": roots_out, "seq_lens": seq_lens, "balance_perm": balance_perm, "inverse_perm": inverse_perm}


@jax.custom_vjp
def low(v):
    return lax.optimization_barrier(v.astype(jnp.bfloat16)).astype(jnp.float32)

@jax.custom_vjp
def low_back(v):
    return v

def low_keep(v):
    return (low(v), None)

def low_pass(kept, grad):
    return (grad,)

def back_keep(v):
    return (v, None)

def back_low(kept, grad):
    return (low(grad),)
low.defvjp(low_keep, low_pass)
low_back.defvjp(back_keep, back_low)
EPSILON = 1e-05
DECAY_RATE = 0.5
LEARN_RATE = 0.2
HIGHEST = lax.Precision.HIGHEST

def matmul_high(left_side, right_side):
    return jnp.dot(left_side, right_side, precision=HIGHEST, preferred_element_type=jnp.float32)

def segment_info(lengths, row_count):
    starts = (jnp.cumsum(lengths) - lengths).astype(jnp.int32)
    row_index = jnp.arange(row_count, dtype=jnp.int32)
    passed = row_index[:, None] >= starts[None, :]
    segment = (lax.optimization_barrier(jnp.sum(passed.astype(jnp.int32), axis=1)) - 1).astype(jnp.int32)
    seq_begin = lax.optimization_barrier(jnp.max(jnp.where(passed, starts[None, :], 0), axis=1)).astype(jnp.int32)
    return (segment, row_index - seq_begin)

def causal_conv(values, kernel, offset_bias, position):
    summed = jnp.zeros_like(values) + offset_bias[None, :]
    for offset in range(KCONV):
        shifted = jnp.pad(values, ((offset, 0), (0, 0)))[:values.shape[0]]
        inside = (position >= offset).astype(jnp.float32)[:, None]
        summed = summed + kernel[offset][None, :] * shifted * inside
    return summed

def block_scan(state_in, operands):
    inner_act, step_len, decay_step, input_map, output_map, segment, alive_mask = operands
    row_order = jnp.arange(segment.shape[0], dtype=jnp.int32)
    cumulative = jnp.cumsum(decay_step, axis=0).T
    allowed = (segment[:, None] == segment[None, :]) & (row_order[:, None] >= row_order[None, :])
    spread = cumulative[:, :, None] - cumulative[:, None, :]
    weights = jnp.where(allowed[None], jnp.exp(jnp.where(allowed[None], spread, 0.0)), 0.0)
    scores = jnp.dot(output_map, input_map.T, precision=HIGHEST, preferred_element_type=jnp.float32)
    driven = step_len[:, :, None] * inner_act
    within = jnp.einsum('hij,jhp->ihp', weights * scores[None], driven, precision=HIGHEST)
    carried = jnp.einsum('in,hpn->ihp', output_map, state_in, precision=HIGHEST)
    carried = carried * (jnp.exp(cumulative).T * alive_mask[:, None])[:, :, None]
    last_sum = cumulative[:, -1]
    same_last = (segment == segment[-1]).astype(jnp.float32)
    toward = jnp.exp(last_sum[None, :] - cumulative.T) * same_last[:, None]
    fresh_state = jnp.einsum('jh,jhp,jn->hpn', toward, driven, input_map, precision=HIGHEST)
    state_out = state_in * (jnp.exp(last_sum) * alive_mask[-1])[:, None, None] + fresh_state
    return (state_out, within + carried)

def mixer_core(gate_proj, inner_proj, state_proj, step_raw, conv_weight, conv_bias, conv_state_weight, conv_state_bias, step_bias, decay_log, skip_gain, segment, position):
    row_count = gate_proj.shape[0]
    head_count = skip_gain.shape[0]
    head_width = gate_proj.shape[1] // head_count
    inner_act = jax.nn.silu(causal_conv(inner_proj, conv_weight, conv_bias, position))
    state_act = jax.nn.silu(causal_conv(state_proj, conv_state_weight, conv_state_bias, position))
    input_map = state_act[:, :STATE]
    output_map = state_act[:, STATE:]
    step_len = jax.nn.softplus(step_raw + step_bias[None, :])
    decay_step = -step_len * jnp.exp(decay_log)[None, :]
    block_count = row_count // SPAN
    seg_blocks = segment.reshape(block_count, SPAN)
    previous = jnp.concatenate([jnp.full((1,), -1, jnp.int32), seg_blocks[:-1, -1].astype(jnp.int32)])
    alive_mask = (seg_blocks == previous[:, None]).astype(jnp.float32)
    start_state = jnp.zeros((head_count, head_width, STATE), jnp.float32)
    operands = (inner_act.reshape(block_count, SPAN, head_count, head_width), step_len.reshape(block_count, SPAN, head_count), decay_step.reshape(block_count, SPAN, head_count), input_map.reshape(block_count, SPAN, STATE), output_map.reshape(block_count, SPAN, STATE), seg_blocks, alive_mask)
    final_state, scanned = lax.scan(jax.checkpoint(block_scan), start_state, operands)
    mixed_out = scanned.reshape(row_count, head_count * head_width) + inner_act * jnp.repeat(skip_gain, head_width)[None, :]
    return mixed_out * jax.nn.silu(gate_proj)

def mixer_group(params, normed, lengths):
    w_gate, w_input, w_state, w_step, conv_weight, conv_bias, conv_state_weight, conv_state_bias, step_bias, decay_log, skip_gain, gate_gain, w_out = params
    segment, position = segment_info(lengths, normed.shape[0])
    gate_proj = low_back(matmul_high(normed, w_gate))
    inner_proj = low_back(matmul_high(normed, w_input))
    state_proj = low_back(matmul_high(normed, w_state))
    step_raw = low_back(matmul_high(normed, w_step))
    gated_out = mixer_core(gate_proj, inner_proj, state_proj, step_raw, conv_weight, conv_bias, conv_state_weight, conv_state_bias, step_bias, decay_log, skip_gain, segment, position)
    square = lax.optimization_barrier(jnp.mean(gated_out * gated_out, axis=1, keepdims=True))
    normal = low(gated_out * lax.rsqrt(square + EPSILON) * gate_gain[None, :])
    return matmul_high(normal, w_out.T)

def shampoo(weight, gradient, stat_pair, root_pair):
    row_count, col_count = gradient.shape
    blocks = gradient.reshape(row_count // BLK, BLK, col_count // BLK, BLK).transpose(0, 2, 1, 3)
    left_stat = jnp.einsum('abij,abkj->abik', blocks, blocks, precision=HIGHEST)
    right_stat = jnp.einsum('abji,abjk->abik', blocks, blocks, precision=HIGHEST)
    fresh_stats = jnp.stack([left_stat, right_stat], axis=2)
    new_stats = DECAY_RATE * stat_pair + (1.0 - DECAY_RATE) * fresh_stats
    turned = jnp.einsum('abij,abjk->abik', root_pair[:, :, 0], blocks, precision=HIGHEST)
    turned = jnp.einsum('abij,abjk->abik', turned, root_pair[:, :, 1], precision=HIGHEST)
    update_step = turned.transpose(0, 2, 1, 3).reshape(row_count, col_count)
    master = weight - LEARN_RATE * update_step
    return (new_stats, master, master.astype(jnp.bfloat16))

def reference(tokens, cotangent, norm_gain, w_gate, w_input, w_state, w_step, conv_weight, conv_bias, conv_state_weight, conv_state_bias, step_bias, decay_log, skip_gain, gate_gain, w_out, stats_gate, stats_input, stats_state, stats_out, roots_gate, roots_input, roots_state, roots_out, seq_lens, balance_perm, inverse_perm):
    weights_in = tuple((member.astype(jnp.float32) for member in (norm_gain, w_gate, w_input, w_state, w_step, conv_weight, conv_bias, conv_state_weight, conv_state_bias, step_bias, decay_log, skip_gain, gate_gain, w_out)))
    tokens_f = tokens.astype(jnp.float32)

    def forward(tokens_v, params):
        square = lax.optimization_barrier(jnp.mean(tokens_v * tokens_v, axis=1, keepdims=True))
        normed = low_back(low(tokens_v * lax.rsqrt(square + EPSILON) * params[0][None, :]))
        ordered = normed[balance_perm].reshape(N_DP, TOK_GRP, D)

        def one_group(operands):
            return mixer_group(params[1:], operands[0], operands[1])
        branch = lax.map(jax.checkpoint(one_group), (ordered, seq_lens))
        branch = low(branch.reshape(TOKENS, D))
        return tokens_v + branch[inverse_perm]
    block_out, back_fn = jax.vjp(forward, tokens_f, weights_in)
    tokens_grad, param_grads = back_fn(cotangent.astype(jnp.float32))
    new_gate = shampoo(weights_in[1], param_grads[1], stats_gate, roots_gate)
    new_input = shampoo(weights_in[2], param_grads[2], stats_input, roots_input)
    new_state = shampoo(weights_in[3], param_grads[3], stats_state, roots_state)
    new_out = shampoo(weights_in[13], param_grads[13], stats_out, roots_out)
    return (block_out, tokens_grad, param_grads[0], param_grads[1], param_grads[2], param_grads[3], param_grads[4], param_grads[5], param_grads[6], param_grads[7], param_grads[8], param_grads[9], param_grads[10], param_grads[11], param_grads[12], param_grads[13], new_gate[0], new_input[0], new_state[0], new_out[0], new_gate[1], new_input[1], new_state[1], new_out[1], new_gate[2], new_input[2], new_state[2], new_out[2])
```

```python
import jax
import jax.numpy as jnp
from jax import lax
from jax.experimental import pallas as pl
from jax.experimental.pallas import tpu as pltpu
from jax.sharding import PartitionSpec as P

D = 2048
STATE = 128
KCONV = 4
SPAN = 256
BLK = 64
INNER = 4096


EPSILON = 1e-05
DECAY_RATE = 0.5
LEARN_RATE = 0.2
HIGHEST = lax.Precision.HIGHEST


def segment_info(lengths, row_count):
    starts = jnp.cumsum(lengths) - lengths
    row_index = jnp.arange(row_count, dtype=jnp.int32)
    passed = row_index[:, None] >= starts[None, :]
    segment = jnp.sum(passed.astype(jnp.int32), axis=1) - 1
    seq_begin = jnp.max(jnp.where(passed, starts[None, :], 0), axis=1)
    return (segment, row_index - seq_begin)


MIX_ROWS = 256
LANES = 256
HEADW = 64
TILEH = LANES // HEADW


def _split3(v):
    hi = v.astype(jnp.bfloat16)
    r1 = v - hi.astype(jnp.float32)
    mid = r1.astype(jnp.bfloat16)
    lo = (r1 - mid.astype(jnp.float32)).astype(jnp.bfloat16)
    return jnp.concatenate([hi, mid, lo], axis=1)


def _dot(a, b):
    return lax.dot_general(a, b, (((1,), (0,)), ((), ())), preferred_element_type=jnp.float32)


def _dot_t(a, b):
    return lax.dot_general(a, b, (((1,), (1,)), ((), ())), preferred_element_type=jnp.float32)


def _dot_tl(a, b):
    return lax.dot_general(a, b, (((0,), (0,)), ((), ())), preferred_element_type=jnp.float32)


def _conv(v, w, b, pos):
    out = w[0:1, :] * v + b
    for k in range(1, KCONV):
        out = out + jnp.where(pos >= k, pltpu.roll(v, k, 0), 0.0) * w[k : k + 1, :]
    return out


def _iota(shape, axis):
    return lax.broadcasted_iota(jnp.int32, shape, axis)


def _lower():
    return _iota((MIX_ROWS, MIX_ROWS), 0) >= _iota((MIX_ROWS, MIX_ROWS), 1)


def _head_masks():
    lane = _iota((1, LANES), 1) // HEADW
    return [(lane == h) for h in range(TILEH)]


def _spread_lanes(cols):
    lane = _iota((1, 2 * HEADW), 1)
    return jnp.concatenate(
        [jnp.where(lane < HEADW, cols[2 * i], cols[2 * i + 1]) for i in range(TILEH // 2)], axis=1
    )


def _decay_terms(dt_b, rate, tri):
    a_b = -dt_b * rate
    parts = _split3(a_b)
    c = _dot(tri, parts)
    cum = c[:, 0:TILEH] + c[:, TILEH : 2 * TILEH] + c[:, 2 * TILEH : 3 * TILEH]
    ct = lax.dot_general(parts, tri, (((0,), (1,)), ((), ())), preferred_element_type=jnp.float32)
    cum_t = ct[0:TILEH] + ct[TILEH : 2 * TILEH] + ct[2 * TILEH : 3 * TILEH]
    cols = [jnp.broadcast_to(cum[:, h : h + 1], (MIX_ROWS, 128)) for h in range(TILEH)]
    return a_b, cols, cum_t


def mixer_fwd_kernel(
    gate_ref, inner_ref, state_ref, dt_ref, rate_ref, cw_ref, cb_ref, csw_ref, csb_ref, skip_ref,
    segc_ref, segr_ref, posc_ref,
    mixed_ref, gated_ref, square_ref,
    bc_ref, bt_ref, s_ref,
):
    rows = inner_ref.shape[0]
    blocks = rows // MIX_ROWS
    pos = posc_ref[...]
    g = pl.program_id(0)

    @pl.when(g == 0)
    def _():
        pre = _conv(state_ref[...], csw_ref[...], csb_ref[...], pos)
        act = pre * jax.nn.sigmoid(pre)
        bc_ref[...] = act.astype(jnp.bfloat16)
        low = _lower()
        for b in range(blocks):
            r = slice(b * MIX_ROWS, (b + 1) * MIX_ROWS)
            bt_ref[:, r] = jnp.transpose(act[r, 0:STATE]).astype(jnp.bfloat16)
            s = _dot_t(bc_ref[r, STATE : 2 * STATE], bc_ref[r, 0:STATE])
            ok = (segc_ref[r, :] == segr_ref[:, r]) & low
            s_ref[b] = jnp.where(ok, s, 0.0)
        square_ref[...] = jnp.zeros_like(square_ref)

    pre = _conv(inner_ref[...], cw_ref[...], cb_ref[...], pos)
    x_all = pre * jax.nn.sigmoid(pre)
    tri = jnp.where(_lower(), 1.0, 0.0).astype(jnp.bfloat16)
    masks = _head_masks()
    rate = rate_ref[0]
    skip = skip_ref[...]
    state = jnp.zeros((STATE, LANES), jnp.float32)
    for b in range(blocks):
        r = slice(b * MIX_ROWS, (b + 1) * MIX_ROWS)
        dt_b = dt_ref[0, r, :]
        x = x_all[r]
        dte = _spread_lanes(
            [jnp.broadcast_to(dt_b[:, h : h + 1], (MIX_ROWS, 128)) for h in range(TILEH)]
        )
        u = dte * x
        ub = u.astype(jnp.bfloat16)
        _, cols, cum_t = _decay_terms(dt_b, rate, tri)
        cume = _spread_lanes(cols)
        seg = segc_ref[r, :]
        y = jnp.zeros((MIX_ROWS, LANES), jnp.float32)
        for h in range(TILEH):
            wide = jnp.concatenate([cols[h], cols[h]], axis=1)
            w = jnp.exp(jnp.minimum(wide - cum_t[h : h + 1, :], 0.0)) * s_ref[b]
            y = y + _dot(w.astype(jnp.bfloat16), jnp.where(masks[h], ub, jnp.zeros_like(ub)))
        if b > 0:
            alive = seg == segc_ref[b * MIX_ROWS - 1 : b * MIX_ROWS, :]
            carried = _dot(bc_ref[r, STATE : 2 * STATE], state.astype(jnp.bfloat16))
            y = y + carried * jnp.where(alive, jnp.exp(cume), 0.0)
        if b < blocks - 1:
            last = cume[MIX_ROWS - 1 : MIX_ROWS, :]
            seg_last = segc_ref[(b + 1) * MIX_ROWS - 1 : (b + 1) * MIX_ROWS, :]
            toward = jnp.where(seg == seg_last, jnp.exp(last - cume), 0.0)
            fresh = _dot(bt_ref[:, r], (toward * u).astype(jnp.bfloat16))
            if b > 0:
                keep = seg_last == segc_ref[b * MIX_ROWS - 1 : b * MIX_ROWS, :]
                state = state * jnp.where(keep, jnp.exp(last), 0.0) + fresh
            else:
                state = fresh
        mixed = y + x * skip
        gate = gate_ref[r, :]
        gated = mixed * (gate * jax.nn.sigmoid(gate))
        mixed_ref[r, :] = mixed
        gated_ref[r, :] = gated
        square_ref[r, :] += jnp.sum(gated * gated, axis=1, keepdims=True)


def mixer_bwd_kernel(
    gate_ref, inner_ref, mixed_ref, dnorm_ref, gs_ref, coef_ref, gain_ref,
    state_ref, dt_ref, sig_ref, rate_ref, cw_ref, cb_ref, csw_ref, csb_ref, skip_ref,
    segc_ref, segr_ref, posc_ref,
    dgate_ref, dinner_ref, dstep_ref, dstate_ref, rowsum_ref, headsum_ref, stsum_ref,
    bc_ref, bt_ref, ct_ref, st_ref, dst_acc, dbc_acc, dpre_ref, keep_ref,
):
    rows = inner_ref.shape[0]
    blocks = rows // MIX_ROWS
    pos = posc_ref[...]
    g = pl.program_id(0)

    @pl.when(g == 0)
    def _():
        pre = _conv(state_ref[...], csw_ref[...], csb_ref[...], pos)
        act = pre * jax.nn.sigmoid(pre)
        bc_ref[...] = act.astype(jnp.bfloat16)
        up = _iota((MIX_ROWS, MIX_ROWS), 0) <= _iota((MIX_ROWS, MIX_ROWS), 1)
        for b in range(blocks):
            r = slice(b * MIX_ROWS, (b + 1) * MIX_ROWS)
            bt_ref[:, r] = jnp.transpose(act[r, 0:STATE]).astype(jnp.bfloat16)
            ct_ref[:, r] = jnp.transpose(act[r, STATE : 2 * STATE]).astype(jnp.bfloat16)
            s = _dot_t(bc_ref[r, 0:STATE], bc_ref[r, STATE : 2 * STATE])
            ok = (segc_ref[r, :] == segr_ref[:, r]) & up
            st_ref[b] = jnp.where(ok, s, 0.0)
        dst_acc[...] = jnp.zeros_like(dst_acc)
        dbc_acc[...] = jnp.zeros_like(dbc_acc)

    inner = inner_ref[...]
    pre = _conv(inner, cw_ref[...], cb_ref[...], pos)
    sg_x = jax.nn.sigmoid(pre)
    x_all = pre * sg_x
    tri = jnp.where(_lower(), 1.0, 0.0).astype(jnp.bfloat16)
    tri_up = jnp.where(
        _iota((MIX_ROWS, MIX_ROWS), 0) <= _iota((MIX_ROWS, MIX_ROWS), 1), 1.0, 0.0
    ).astype(jnp.bfloat16)
    masks = _head_masks()
    pick = jnp.where(
        _iota((LANES, TILEH), 0) // HEADW == _iota((LANES, TILEH), 1), 1.0, 0.0
    ).astype(jnp.bfloat16)
    rate = rate_ref[0]
    skip = skip_ref[...]
    gain = gain_ref[...]

    def per_head(v):
        hi = v.astype(jnp.bfloat16)
        lo = (v - hi.astype(jnp.float32)).astype(jnp.bfloat16)
        return _dot(hi, pick) + _dot(lo, pick)

    def entry_of(b):
        r = slice(b * MIX_ROWS, (b + 1) * MIX_ROWS)
        dt_b = dt_ref[0, r, :]
        dte = _spread_lanes(
            [jnp.broadcast_to(dt_b[:, h : h + 1], (MIX_ROWS, 128)) for h in range(TILEH)]
        )
        a_b, cols, cum_t = _decay_terms(dt_b, rate, tri)
        cume = _spread_lanes(cols)
        u = dte * x_all[r]
        seg = segc_ref[r, :]
        entry = dict(a=a_b, dte=dte, cols=cols, cum_t=cum_t, ub=u.astype(jnp.bfloat16))
        prev = segc_ref[b * MIX_ROWS - 1 : b * MIX_ROWS, :] if b > 0 else None
        if b > 0:
            entry["e"] = jnp.where(seg == prev, jnp.exp(cume), 0.0)
        if b < blocks - 1:
            last = cume[MIX_ROWS - 1 : MIX_ROWS, :]
            seg_last = segc_ref[(b + 1) * MIX_ROWS - 1 : (b + 1) * MIX_ROWS, :]
            entry["t"] = jnp.where(seg == seg_last, jnp.exp(last - cume), 0.0)
            entry["tub"] = (entry["t"] * u).astype(jnp.bfloat16)
            if b > 0:
                entry["d"] = jnp.where(seg_last == prev, jnp.exp(last), 0.0)
        return entry

    terms = []
    state = None
    for b in range(blocks):
        r = slice(b * MIX_ROWS, (b + 1) * MIX_ROWS)
        entry = entry_of(b)
        if b > 0:
            keep_ref[b - 1] = state
        if b < blocks - 1:
            fresh = _dot(bt_ref[:, r], entry["tub"])
            state = state * entry["d"] + fresh if b > 0 else fresh
        terms.append(entry if blocks <= 4 else None)

    skip_row = jnp.zeros((1, LANES), jnp.float32)
    gain_row = jnp.zeros((1, LANES), jnp.float32)
    bias_head = jnp.zeros((1, TILEH), jnp.float32)
    rate_head = jnp.zeros((1, TILEH), jnp.float32)
    dst = None
    for b in reversed(range(blocks)):
        r = slice(b * MIX_ROWS, (b + 1) * MIX_ROWS)
        tm = terms[b] or entry_of(b)
        x = x_all[r]
        ub = tm["ub"]
        gate = gate_ref[r, :]
        sg = jax.nn.sigmoid(gate)
        silu = gate * sg
        mixed = mixed_ref[r, :]
        gated = mixed * silu
        dn = dnorm_ref[r, :] * gs_ref[r, :]
        dg = dn * gain - gated * coef_ref[r, :]
        gain_row = gain_row + jnp.sum(dn * gated, axis=0, keepdims=True)
        dgate_ref[r, :] = (dg * mixed * (sg + silu * (1.0 - sg))).astype(jnp.bfloat16)
        dm = dg * silu
        dyb = dm.astype(jnp.bfloat16)
        skip_row = skip_row + jnp.sum(dm * x, axis=0, keepdims=True)
        du = jnp.zeros((MIX_ROWS, LANES), jnp.float32)
        dst_sum = jnp.zeros((MIX_ROWS, MIX_ROWS), jnp.float32)
        for h in range(TILEH):
            wide = jnp.concatenate([tm["cols"][h], tm["cols"][h]], axis=1)
            lt = jnp.exp(jnp.minimum(tm["cum_t"][h : h + 1, :] - wide, 0.0))
            wt = (lt * st_ref[b]).astype(jnp.bfloat16)
            dyh = jnp.where(masks[h], dyb, jnp.zeros_like(dyb))
            du = du + _dot(wt, dyh)
            dst_sum = dst_sum + lt * _dot_t(ub, dyh)
        dst_acc[b] += dst_sum
        ubf = ub.astype(jnp.float32)
        tail = None
        if b < blocks - 1:
            dstb = dst.astype(jnp.bfloat16)
            duf = tm["t"] * _dot(bc_ref[r, 0:STATE], dstb)
            dbc_acc[r, 0:STATE] += _dot_t(tm["tub"], dstb)
            tail = jnp.sum(ubf * duf, axis=0, keepdims=True)
            if b > 0:
                tail = tail + jnp.sum(dst * keep_ref[b - 1], axis=0, keepdims=True) * tm["d"]
            du = du + duf
        y = mixed - x * skip
        z = dyb.astype(jnp.float32) * y - ubf * du
        if tail is not None:
            z = z + jnp.where(_iota((MIX_ROWS, 1), 0) == MIX_ROWS - 1, tail, 0.0)
        if b > 0:
            edy = (tm["e"] * dm).astype(jnp.bfloat16)
            dbc_acc[r, STATE : 2 * STATE] += _dot_t(edy, keep_ref[b - 1].astype(jnp.bfloat16))
            step = _dot(ct_ref[:, r], edy)
            if b < blocks - 1:
                dst = dst * tm["d"] + step
            else:
                dst = step
        c = _dot(tri_up, _split3(per_head(z)))
        da = c[:, 0:TILEH] + c[:, TILEH : 2 * TILEH] + c[:, 2 * TILEH : 3 * TILEH]
        ddt = per_head(du * x) - da * rate
        dsr = ddt * sig_ref[0, r, :]
        dstep_ref[0, r, :] = dsr
        bias_head = bias_head + jnp.sum(dsr, axis=0, keepdims=True)
        rate_head = rate_head + jnp.sum(da * tm["a"], axis=0, keepdims=True)
        s_b = sg_x[r]
        dpre_ref[r, :] = (tm["dte"] * du + skip * dm) * (s_b + x * (1.0 - s_b))

    def conv_back(dpre, v, w):
        out = w[0:1, :] * dpre
        sums = [jnp.sum(dpre * v, axis=0, keepdims=True)]
        for k in range(1, KCONV):
            held = jnp.where(pos >= k, dpre, 0.0)
            out = out + w[k : k + 1, :] * pltpu.roll(held, rows - k, 0)
            sums.append(jnp.sum(held * pltpu.roll(v, k, 0), axis=0, keepdims=True))
        sums.append(jnp.sum(dpre, axis=0, keepdims=True))
        return out, sums

    din, sums = conv_back(dpre_ref[...], inner, cw_ref[...])
    dinner_ref[...] = din.astype(jnp.bfloat16)
    rowsum_ref[...] = jnp.concatenate(
        sums + [gain_row, skip_row, jnp.zeros((1, LANES), jnp.float32)], axis=0
    )
    headsum_ref[0] = jnp.concatenate([bias_head, rate_head], axis=0)

    @pl.when(g == pl.num_programs(0) - 1)
    def _():
        up = _iota((MIX_ROWS, MIX_ROWS), 0) <= _iota((MIX_ROWS, MIX_ROWS), 1)
        for b in range(blocks):
            r = slice(b * MIX_ROWS, (b + 1) * MIX_ROWS)
            ok = (segc_ref[r, :] == segr_ref[:, r]) & up
            ds = jnp.where(ok, dst_acc[b], 0.0).astype(jnp.bfloat16)
            dbc_acc[r, 0:STATE] += _dot(ds, bc_ref[r, STATE : 2 * STATE])
            dbc_acc[r, STATE : 2 * STATE] += _dot_tl(ds, bc_ref[r, 0:STATE])
        sp = state_ref[...]
        pre_s = _conv(sp, csw_ref[...], csb_ref[...], pos)
        sg_s = jax.nn.sigmoid(pre_s)
        dpre_s = dbc_acc[...] * (sg_s + pre_s * sg_s * (1.0 - sg_s))
        dsp, sums_s = conv_back(dpre_s, sp, csw_ref[...])
        dstate_ref[...] = dsp.astype(jnp.bfloat16)
        stsum_ref[...] = jnp.concatenate(
            sums_s + [jnp.zeros((3, 2 * STATE), jnp.float32)], axis=0
        )


def _tile(rows):
    if rows > 4 * MIX_ROWS:
        return pl.BlockSpec((rows, LANES), lambda g: (0, g), pipeline_mode=pl.Buffered(1))
    return pl.BlockSpec((rows, LANES), lambda g: (0, g))


def _whole(shape):
    return pl.BlockSpec(shape, lambda g: (0,) * len(shape))


def _heads(rows):
    return pl.BlockSpec((1, rows, TILEH), lambda g: (g, 0, 0))


def mixer_consts(conv_w, conv_b, csw, csb, skip, decay_log, segment, position):
    f = jnp.float32
    head_count = skip.shape[0]
    return dict(
        rate=jnp.exp(decay_log.astype(f)).reshape(head_count // TILEH, 1, TILEH),
        cw=conv_w.astype(f), cb=conv_b.astype(f)[None, :], csw=csw.astype(f), csb=csb.astype(f)[None, :],
        skip=jnp.repeat(skip.astype(f), HEADW)[None, :],
        segc=segment[:, None], segr=segment[None, :], posc=position[:, None],
    )


def mixer_forward(gate, inner, state, dt, k):
    rows, width = inner.shape
    blocks = rows // MIX_ROWS
    f = jnp.float32
    wide = jax.ShapeDtypeStruct((rows, width), f)
    return pl.pallas_call(
        mixer_fwd_kernel,
        grid=(width // LANES,),
        in_specs=[
            _tile(rows), _tile(rows), _whole((rows, 2 * STATE)), _heads(rows), _heads(1),
            _tile(KCONV), _tile(1), _whole((KCONV, 2 * STATE)), _whole((1, 2 * STATE)), _tile(1),
            _whole((rows, 1)), _whole((1, rows)), _whole((rows, 1)),
        ],
        out_specs=[_tile(rows), _tile(rows), _whole((rows, 1))],
        out_shape=[wide, wide, jax.ShapeDtypeStruct((rows, 1), f)],
        scratch_shapes=[
            pltpu.VMEM((rows, 2 * STATE), jnp.bfloat16),
            pltpu.VMEM((STATE, rows), jnp.bfloat16),
            pltpu.VMEM((blocks, MIX_ROWS, MIX_ROWS), f),
        ],
        name="mixer_forward",
    )(gate, inner, state, dt, k["rate"], k["cw"], k["cb"], k["csw"], k["csb"], k["skip"],
      k["segc"], k["segr"], k["posc"])


def mixer_backward(gate, inner, mixed, dnorm, gs, coef, gain, state, dt, sig, k):
    rows, width = inner.shape
    blocks = rows // MIX_ROWS
    tiles = width // LANES
    f = jnp.float32
    wide = jax.ShapeDtypeStruct((rows, width), jnp.bfloat16)
    return pl.pallas_call(
        mixer_bwd_kernel,
        grid=(tiles,),
        in_specs=[
            _tile(rows), _tile(rows), _tile(rows), _tile(rows), _whole((rows, 1)), _whole((rows, 1)), _tile(1),
            _whole((rows, 2 * STATE)), _heads(rows), _heads(rows), _heads(1),
            _tile(KCONV), _tile(1), _whole((KCONV, 2 * STATE)), _whole((1, 2 * STATE)), _tile(1),
            _whole((rows, 1)), _whole((1, rows)), _whole((rows, 1)),
        ],
        out_specs=[
            _tile(rows), _tile(rows), _heads(rows), _whole((rows, 2 * STATE)),
            _tile(8), _heads(2), _whole((8, 2 * STATE)),
        ],
        out_shape=[
            wide, wide, jax.ShapeDtypeStruct((tiles, rows, TILEH), f),
            jax.ShapeDtypeStruct((rows, 2 * STATE), jnp.bfloat16),
            jax.ShapeDtypeStruct((8, width), f), jax.ShapeDtypeStruct((tiles, 2, TILEH), f),
            jax.ShapeDtypeStruct((8, 2 * STATE), f),
        ],
        scratch_shapes=[
            pltpu.VMEM((rows, 2 * STATE), jnp.bfloat16),
            pltpu.VMEM((STATE, rows), jnp.bfloat16),
            pltpu.VMEM((STATE, rows), jnp.bfloat16),
            pltpu.VMEM((blocks, MIX_ROWS, MIX_ROWS), f),
            pltpu.VMEM((blocks, MIX_ROWS, MIX_ROWS), f),
            pltpu.VMEM((rows, 2 * STATE), f),
            pltpu.VMEM((rows, LANES), f),
            pltpu.VMEM((max(blocks - 1, 1), STATE, LANES), f),
        ],
        name="mixer_backward",
    )(gate, inner, mixed, dnorm, gs, coef, gain, state, dt, sig, k["rate"], k["cw"], k["cb"], k["csw"], k["csb"], k["skip"],
      k["segc"], k["segr"], k["posc"])


def shampoo(weight, gradient, stat_pair, root_pair):
    row_count, col_count = gradient.shape
    blocks = gradient.reshape(row_count // BLK, BLK, col_count // BLK, BLK).transpose(0, 2, 1, 3)
    left_stat = jnp.einsum("abij,abkj->abik", blocks, blocks, precision=HIGHEST)
    right_stat = jnp.einsum("abji,abjk->abik", blocks, blocks, precision=HIGHEST)
    fresh_stats = jnp.stack([left_stat, right_stat], axis=2)
    new_stats = DECAY_RATE * stat_pair + (1.0 - DECAY_RATE) * fresh_stats
    turned = jnp.einsum("abij,abjk->abik", root_pair[:, :, 0], blocks, precision=HIGHEST)
    turned = jnp.einsum("abij,abjk->abik", turned, root_pair[:, :, 1], precision=HIGHEST)
    update_step = turned.transpose(0, 2, 1, 3).reshape(row_count, col_count)
    master = weight - LEARN_RATE * update_step
    return (new_stats, master, master.astype(jnp.bfloat16))


def contract_rows(left_side, right_side):
    return lax.dot_general(
        left_side, right_side, (((0,), (0,)), ((), ())), preferred_element_type=jnp.float32
    )


def contract_cols(left_side, right_side):
    return lax.dot_general(
        left_side, right_side, (((1,), (1,)), ((), ())), preferred_element_type=jnp.float32
    )


def rank_matrix(keys):
    count = keys.shape[0]
    rank = jnp.sum((keys[None, :] < keys[:, None]).astype(jnp.int32), axis=1)
    return (jnp.arange(count, dtype=jnp.int32)[:, None] == rank[None, :]).astype(jnp.bfloat16)


def move_rows(choose, values):
    return jnp.dot(choose, values, preferred_element_type=jnp.float32).astype(jnp.bfloat16)


def move_back(choose, values):
    return lax.dot_general(
        choose, values, (((0,), (0,)), ((), ())), preferred_element_type=jnp.float32
    ).astype(jnp.bfloat16)


def body(
    tokens,
    cotangent,
    norm_gain,
    w_gate,
    w_input,
    w_state,
    w_step,
    conv_weight,
    conv_bias,
    conv_state_weight,
    conv_state_bias,
    step_bias,
    decay_log,
    skip_gain,
    gate_gain,
    w_out,
    stats_gate,
    stats_input,
    stats_state,
    stats_out,
    roots_gate,
    roots_input,
    roots_state,
    roots_out,
    seq_lens,
    balance_perm,
    inverse_perm,
):
    groups = lax.axis_size("dp")
    tensor_ranks = lax.axis_size("tensor")
    local_rows = tokens.shape[0]
    slot_rows = local_rows // groups
    group_rows = local_rows * tensor_ranks
    tokens_f = tokens.astype(jnp.float32)
    scale_in = lax.rsqrt(jnp.mean(tokens_f * tokens_f, axis=1) + EPSILON)
    gain_in = norm_gain.astype(jnp.float32)
    normed = (tokens_f * scale_in[:, None] * gain_in[None, :]).astype(jnp.bfloat16)
    send_choose = rank_matrix(inverse_perm)
    arrived = (
        lax.all_to_all(
            move_rows(send_choose, normed).reshape(groups, slot_rows, D),
            "dp",
            split_axis=0,
            concat_axis=0,
            tiled=True,
        ),
        lax.all_to_all(
            move_rows(send_choose, cotangent).reshape(groups, slot_rows, D),
            "dp",
            split_axis=0,
            concat_axis=0,
            tiled=True,
        ),
    )
    collected = (
        lax.all_gather(arrived[0], "tensor", axis=0, tiled=True),
        lax.all_gather(arrived[1], "tensor", axis=0, tiled=True),
    )
    source = balance_perm // local_rows
    row_key = (source % tensor_ranks * groups + source // tensor_ranks) * group_rows + jnp.arange(
        group_rows, dtype=jnp.int32
    )
    place = rank_matrix(row_key)
    normed_bal = move_back(place, collected[0].reshape(group_rows, D))
    cot_bal = move_back(place, collected[1].reshape(group_rows, D))
    segment, position = segment_info(seq_lens[0], group_rows)
    pieces = (
        lax.all_gather(w_gate, "dp", axis=0, tiled=True),
        lax.all_gather(w_input, "dp", axis=0, tiled=True),
        lax.all_gather(w_state, "dp", axis=0, tiled=True),
        lax.all_gather(w_step, "dp", axis=0, tiled=True),
    )
    columns = normed_bal
    gate_proj, inner_proj, state_proj, step_raw = tuple(
        (
            jnp.dot(columns, pieces[member], preferred_element_type=jnp.float32)
            for member in range(4)
        )
    )

    step_full = step_raw + step_bias.astype(jnp.float32)[None, :]
    tiles = step_full.shape[1] // TILEH
    step_tiles = step_full.reshape(group_rows, tiles, TILEH).transpose(1, 0, 2)
    step_len = jax.nn.softplus(step_tiles)
    step_slope = jax.nn.sigmoid(step_tiles)
    consts = mixer_consts(
        conv_weight, conv_bias, conv_state_weight, conv_state_bias, skip_gain, decay_log, segment, position
    )
    mixed, gated_out, square = mixer_forward(gate_proj, inner_proj, state_proj, step_len, consts)
    whole_square = lax.psum(square[:, 0], "tensor")
    gate_scale = lax.rsqrt(whole_square / INNER + EPSILON)
    gain_gate = gate_gain.astype(jnp.float32)
    normal = (gated_out * gate_scale[:, None] * gain_gate[None, :]).astype(jnp.bfloat16)
    partial_out = contract_cols(normal, lax.all_gather(w_out, "dp", axis=0, tiled=True))
    w_out_part = contract_rows(cot_bal, normal)
    columns = cot_bal
    d_normal = jnp.dot(
        columns, lax.all_gather(w_out, "dp", axis=0, tiled=True), preferred_element_type=jnp.float32
    )
    dot_total = lax.psum(jnp.sum(gated_out * gain_gate[None, :] * d_normal, axis=1), "tensor")
    d_gate, d_inner, d_step, d_state, row_sums, head_sums, state_sums = mixer_backward(
        gate_proj, inner_proj, mixed, d_normal, gate_scale[:, None],
        (gate_scale**3 * dot_total / INNER)[:, None], gain_gate[None, :],
        state_proj, step_len, step_slope, consts,
    )
    d_step = d_step.transpose(1, 0, 2).reshape(group_rows, tiles * TILEH).astype(jnp.bfloat16)
    summed_grads = (
        lax.psum_scatter(
            contract_rows(normed_bal, d_gate).astype(jnp.bfloat16),
            "dp",
            scatter_dimension=0,
            tiled=True,
        ).astype(jnp.float32),
        lax.psum_scatter(
            contract_rows(normed_bal, d_inner).astype(jnp.bfloat16),
            "dp",
            scatter_dimension=0,
            tiled=True,
        ).astype(jnp.float32),
        lax.psum_scatter(
            contract_rows(normed_bal, d_state).astype(jnp.bfloat16),
            "dp",
            scatter_dimension=0,
            tiled=True,
        ).astype(jnp.float32),
        lax.psum_scatter(
            contract_rows(normed_bal, d_step).astype(jnp.bfloat16),
            "dp",
            scatter_dimension=0,
            tiled=True,
        ).astype(jnp.float32),
        lax.psum_scatter(
            w_out_part.astype(jnp.bfloat16), "dp", scatter_dimension=0, tiled=True
        ).astype(jnp.float32),
    )
    pieces = (
        lax.all_gather(w_gate, "dp", axis=0, tiled=True),
        lax.all_gather(w_input, "dp", axis=0, tiled=True),
        lax.all_gather(w_state, "dp", axis=0, tiled=True),
        lax.all_gather(w_step, "dp", axis=0, tiled=True),
    )
    column_term = (
        contract_cols(d_gate, pieces[0])
        + contract_cols(d_inner, pieces[1])
        + contract_cols(d_state, pieces[2])
        + contract_cols(d_step, pieces[3])
    )
    row_totals = (
        lax.psum_scatter(
            move_rows(place, partial_out.astype(jnp.bfloat16)), "tensor", scatter_dimension=0, tiled=True
        ).astype(jnp.float32),
        lax.psum_scatter(
            move_rows(place, column_term.astype(jnp.bfloat16)), "tensor", scatter_dimension=0, tiled=True
        ).astype(jnp.float32),
    )
    returning = (
        lax.all_to_all(
            row_totals[0].astype(jnp.bfloat16).reshape(groups, slot_rows, D),
            "dp",
            split_axis=0,
            concat_axis=0,
            tiled=True,
        ),
        lax.all_to_all(
            row_totals[1].astype(jnp.bfloat16).reshape(groups, slot_rows, D),
            "dp",
            split_axis=0,
            concat_axis=0,
            tiled=True,
        ),
    )
    branch = move_back(send_choose, returning[0].reshape(local_rows, D)).astype(jnp.float32)
    d_tokens_normed = move_back(send_choose, returning[1].reshape(local_rows, D)).astype(jnp.float32)
    block_out = tokens_f + branch
    norm_gain_part = jnp.sum(d_tokens_normed * tokens_f * scale_in[:, None], axis=0)
    dot_in = jnp.sum(tokens_f * gain_in[None, :] * d_tokens_normed, axis=1)
    tokens_grad = (
        cotangent.astype(jnp.float32)
        + d_tokens_normed * scale_in[:, None] * gain_in[None, :]
        - tokens_f * (scale_in**3 * dot_in / D)[:, None]
    )
    over_groups = lax.psum(
        (
            norm_gain_part,
            state_sums[:KCONV],
            state_sums[KCONV],
            row_sums[:KCONV],
            row_sums[KCONV],
            head_sums[:, 0].reshape(-1),
            head_sums[:, 1].reshape(-1),
            row_sums[KCONV + 2].reshape(-1, HEADW).sum(axis=1),
            row_sums[KCONV + 1],
        ),
        "dp",
    )
    over_ranks = (
        lax.psum(summed_grads[2].astype(jnp.bfloat16), "tensor").astype(jnp.float32),
        lax.psum(over_groups[0].astype(jnp.bfloat16), "tensor").astype(jnp.float32),
        lax.psum(over_groups[1].astype(jnp.bfloat16), "tensor").astype(jnp.float32),
        lax.psum(over_groups[2].astype(jnp.bfloat16), "tensor").astype(jnp.float32),
    )
    new_gate = shampoo(w_gate.astype(jnp.float32), summed_grads[0], stats_gate, roots_gate)
    new_input = shampoo(w_input.astype(jnp.float32), summed_grads[1], stats_input, roots_input)
    new_state = shampoo(w_state.astype(jnp.float32), over_ranks[0], stats_state, roots_state)
    new_out = shampoo(w_out.astype(jnp.float32), summed_grads[4], stats_out, roots_out)
    return (
        block_out,
        tokens_grad,
        over_ranks[1],
        summed_grads[0],
        summed_grads[1],
        over_ranks[0],
        summed_grads[3],
        over_groups[3],
        over_groups[4],
        over_ranks[2],
        over_ranks[3],
        over_groups[5],
        over_groups[6],
        over_groups[7],
        over_groups[8],
        summed_grads[4],
        new_gate[0],
        new_input[0],
        new_state[0],
        new_out[0],
        new_gate[1],
        new_input[1],
        new_state[1],
        new_out[1],
        new_gate[2],
        new_input[2],
        new_state[2],
        new_out[2],
    )


def solution(mesh):
    placed = (
        P(("dp", "tensor"), None),
        P(("dp", "tensor"), None),
        P(),
        P("dp", "tensor"),
        P("dp", "tensor"),
        P("dp", None),
        P("dp", "tensor"),
        P(None, "tensor"),
        P("tensor"),
        P(),
        P(),
        P("tensor"),
        P("tensor"),
        P("tensor"),
        P("tensor"),
        P("dp", "tensor"),
        P("dp", "tensor", None, None, None),
        P("dp", "tensor", None, None, None),
        P("dp", None, None, None, None),
        P("dp", "tensor", None, None, None),
        P("dp", "tensor", None, None, None),
        P("dp", "tensor", None, None, None),
        P("dp", None, None, None, None),
        P("dp", "tensor", None, None, None),
        P("dp", None),
        P("dp"),
        P(("dp", "tensor")),
    )
    return jax.shard_map(
        body,
        mesh=mesh,
        in_specs=placed,
        out_specs=(
            P(("dp", "tensor"), None),
            P(("dp", "tensor"), None),
            P(),
            P("dp", "tensor"),
            P("dp", "tensor"),
            P("dp", None),
            P("dp", "tensor"),
            P(None, "tensor"),
            P("tensor"),
            P(),
            P(),
            P("tensor"),
            P("tensor"),
            P("tensor"),
            P("tensor"),
            P("dp", "tensor"),
            P("dp", "tensor", None, None, None),
            P("dp", "tensor", None, None, None),
            P("dp", None, None, None, None),
            P("dp", "tensor", None, None, None),
            P("dp", "tensor"),
            P("dp", "tensor"),
            P("dp", None),
            P("dp", "tensor"),
            P("dp", "tensor"),
            P("dp", "tensor"),
            P("dp", None),
            P("dp", "tensor"),
        ),
        check_vma=False,
    )
```

```python
import jax
import jax.numpy as jnp
from jax import lax
from jax.experimental import pallas as pl
from jax.experimental.pallas import tpu as pltpu
from jax.sharding import PartitionSpec as P

D = 2048
STATE = 128
KCONV = 4
SPAN = 256
BLK = 64
INNER = 4096


EPSILON = 1e-05
DECAY_RATE = 0.5
LEARN_RATE = 0.2
HIGHEST = lax.Precision.HIGHEST


def segment_info(lengths, row_count):
    starts = jnp.cumsum(lengths) - lengths
    row_index = jnp.arange(row_count, dtype=jnp.int32)
    passed = row_index[:, None] >= starts[None, :]
    segment = jnp.sum(passed.astype(jnp.int32), axis=1) - 1
    seq_begin = jnp.max(jnp.where(passed, starts[None, :], 0), axis=1)
    return (segment, row_index - seq_begin)


MIX_ROWS = 256
LANES = 256
HEADW = 64
TILEH = LANES // HEADW


def _split3(v):
    hi = v.astype(jnp.bfloat16)
    r1 = v - hi.astype(jnp.float32)
    mid = r1.astype(jnp.bfloat16)
    lo = (r1 - mid.astype(jnp.float32)).astype(jnp.bfloat16)
    return jnp.concatenate([hi, mid, lo], axis=1)


def _dot(a, b):
    return lax.dot_general(a, b, (((1,), (0,)), ((), ())), preferred_element_type=jnp.float32)


def _dot_t(a, b):
    return lax.dot_general(a, b, (((1,), (1,)), ((), ())), preferred_element_type=jnp.float32)


def _dot_tl(a, b):
    return lax.dot_general(a, b, (((0,), (0,)), ((), ())), preferred_element_type=jnp.float32)


def _conv(v, w, b, pos):
    out = w[0:1, :] * v + b
    for k in range(1, KCONV):
        out = out + jnp.where(pos >= k, pltpu.roll(v, k, 0), 0.0) * w[k : k + 1, :]
    return out


def _iota(shape, axis):
    return lax.broadcasted_iota(jnp.int32, shape, axis)


def _lower():
    return _iota((MIX_ROWS, MIX_ROWS), 0) >= _iota((MIX_ROWS, MIX_ROWS), 1)


def _head_masks():
    lane = _iota((1, LANES), 1) // HEADW
    return [(lane == h) for h in range(TILEH)]


def _spread_lanes(cols):
    lane = _iota((1, 2 * HEADW), 1)
    return jnp.concatenate(
        [jnp.where(lane < HEADW, cols[2 * i], cols[2 * i + 1]) for i in range(TILEH // 2)], axis=1
    )


def _decay_terms(dt_b, rate, tri):
    a_b = -dt_b * rate
    parts = _split3(a_b)
    c = _dot(tri, parts)
    cum = c[:, 0:TILEH] + c[:, TILEH : 2 * TILEH] + c[:, 2 * TILEH : 3 * TILEH]
    ct = lax.dot_general(parts, tri, (((0,), (1,)), ((), ())), preferred_element_type=jnp.float32)
    cum_t = ct[0:TILEH] + ct[TILEH : 2 * TILEH] + ct[2 * TILEH : 3 * TILEH]
    cols = [jnp.broadcast_to(cum[:, h : h + 1], (MIX_ROWS, 128)) for h in range(TILEH)]
    return a_b, cols, cum_t


def mixer_fwd_kernel(
    gate_ref, inner_ref, state_ref, dt_ref, rate_ref, cw_ref, cb_ref, csw_ref, csb_ref, skip_ref,
    segc_ref, segr_ref, posc_ref,
    mixed_ref, gated_ref, square_ref,
    bc_ref, bt_ref, s_ref,
):
    rows = inner_ref.shape[0]
    blocks = rows // MIX_ROWS
    pos = posc_ref[...]
    g = pl.program_id(1)

    @pl.when(g == 0)
    def _():
        pre = _conv(state_ref[...], csw_ref[...], csb_ref[...], pos)
        act = pre * jax.nn.sigmoid(pre)
        bc_ref[...] = act.astype(jnp.bfloat16)
        low = _lower()
        for b in range(blocks):
            r = slice(b * MIX_ROWS, (b + 1) * MIX_ROWS)
            bt_ref[:, r] = jnp.transpose(act[r, 0:STATE]).astype(jnp.bfloat16)
            s = _dot_t(bc_ref[r, STATE : 2 * STATE], bc_ref[r, 0:STATE])
            ok = (segc_ref[r, :] == segr_ref[:, r]) & low
            s_ref[b] = jnp.where(ok, s, 0.0)
        square_ref[...] = jnp.zeros_like(square_ref)

    pre = _conv(inner_ref[...], cw_ref[...], cb_ref[...], pos)
    x_all = pre * jax.nn.sigmoid(pre)
    tri = jnp.where(_lower(), 1.0, 0.0).astype(jnp.bfloat16)
    masks = _head_masks()
    rate = rate_ref[0]
    skip = skip_ref[...]
    state = jnp.zeros((STATE, LANES), jnp.float32)
    for b in range(blocks):
        r = slice(b * MIX_ROWS, (b + 1) * MIX_ROWS)
        dt_b = dt_ref[0, r, :]
        x = x_all[r]
        dte = _spread_lanes(
            [jnp.broadcast_to(dt_b[:, h : h + 1], (MIX_ROWS, 128)) for h in range(TILEH)]
        )
        u = dte * x
        ub = u.astype(jnp.bfloat16)
        _, cols, cum_t = _decay_terms(dt_b, rate, tri)
        cume = _spread_lanes(cols)
        seg = segc_ref[r, :]
        y = jnp.zeros((MIX_ROWS, LANES), jnp.float32)
        for h in range(TILEH):
            wide = jnp.concatenate([cols[h], cols[h]], axis=1)
            w = jnp.exp(jnp.minimum(wide - cum_t[h : h + 1, :], 0.0)) * s_ref[b]
            y = y + _dot(w.astype(jnp.bfloat16), jnp.where(masks[h], ub, jnp.zeros_like(ub)))
        if b > 0:
            alive = seg == segc_ref[b * MIX_ROWS - 1 : b * MIX_ROWS, :]
            carried = _dot(bc_ref[r, STATE : 2 * STATE], state.astype(jnp.bfloat16))
            y = y + carried * jnp.where(alive, jnp.exp(cume), 0.0)
        if b < blocks - 1:
            last = cume[MIX_ROWS - 1 : MIX_ROWS, :]
            seg_last = segc_ref[(b + 1) * MIX_ROWS - 1 : (b + 1) * MIX_ROWS, :]
            toward = jnp.where(seg == seg_last, jnp.exp(last - cume), 0.0)
            fresh = _dot(bt_ref[:, r], (toward * u).astype(jnp.bfloat16))
            if b > 0:
                keep = seg_last == segc_ref[b * MIX_ROWS - 1 : b * MIX_ROWS, :]
                state = state * jnp.where(keep, jnp.exp(last), 0.0) + fresh
            else:
                state = fresh
        mixed = y + x * skip
        gate = gate_ref[r, :]
        gated = mixed * (gate * jax.nn.sigmoid(gate))
        mixed_ref[r, :] = mixed
        gated_ref[r, :] = gated
        square_ref[r, :] += jnp.sum(gated * gated, axis=1, keepdims=True)


def mixer_bwd_kernel(
    gate_ref, inner_ref, mixed_ref, dnorm_ref, gs_ref, coef_ref, gain_ref,
    state_ref, dt_ref, sig_ref, rate_ref, cw_ref, cb_ref, csw_ref, csb_ref, skip_ref,
    segc_ref, segr_ref, posc_ref,
    dgate_ref, dinner_ref, dstep_ref, dstate_ref, rowsum_ref, headsum_ref, stsum_ref,
    bc_ref, bt_ref, ct_ref, st_ref, dst_acc, dbc_acc, dpre_ref, keep_ref,
):
    rows = inner_ref.shape[0]
    blocks = rows // MIX_ROWS
    pos = posc_ref[...]
    g = pl.program_id(1)

    @pl.when(g == 0)
    def _():
        pre = _conv(state_ref[...], csw_ref[...], csb_ref[...], pos)
        act = pre * jax.nn.sigmoid(pre)
        bc_ref[...] = act.astype(jnp.bfloat16)
        up = _iota((MIX_ROWS, MIX_ROWS), 0) <= _iota((MIX_ROWS, MIX_ROWS), 1)
        for b in range(blocks):
            r = slice(b * MIX_ROWS, (b + 1) * MIX_ROWS)
            bt_ref[:, r] = jnp.transpose(act[r, 0:STATE]).astype(jnp.bfloat16)
            ct_ref[:, r] = jnp.transpose(act[r, STATE : 2 * STATE]).astype(jnp.bfloat16)
            s = _dot_t(bc_ref[r, 0:STATE], bc_ref[r, STATE : 2 * STATE])
            ok = (segc_ref[r, :] == segr_ref[:, r]) & up
            st_ref[b] = jnp.where(ok, s, 0.0)
        dst_acc[...] = jnp.zeros_like(dst_acc)
        dbc_acc[...] = jnp.zeros_like(dbc_acc)

    inner = inner_ref[...]
    pre = _conv(inner, cw_ref[...], cb_ref[...], pos)
    sg_x = jax.nn.sigmoid(pre)
    x_all = pre * sg_x
    tri = jnp.where(_lower(), 1.0, 0.0).astype(jnp.bfloat16)
    tri_up = jnp.where(
        _iota((MIX_ROWS, MIX_ROWS), 0) <= _iota((MIX_ROWS, MIX_ROWS), 1), 1.0, 0.0
    ).astype(jnp.bfloat16)
    masks = _head_masks()
    pick = jnp.where(
        _iota((LANES, TILEH), 0) // HEADW == _iota((LANES, TILEH), 1), 1.0, 0.0
    ).astype(jnp.bfloat16)
    rate = rate_ref[0]
    skip = skip_ref[...]
    gain = gain_ref[...]

    def per_head(v):
        hi = v.astype(jnp.bfloat16)
        lo = (v - hi.astype(jnp.float32)).astype(jnp.bfloat16)
        return _dot(hi, pick) + _dot(lo, pick)

    def entry_of(b):
        r = slice(b * MIX_ROWS, (b + 1) * MIX_ROWS)
        dt_b = dt_ref[0, r, :]
        dte = _spread_lanes(
            [jnp.broadcast_to(dt_b[:, h : h + 1], (MIX_ROWS, 128)) for h in range(TILEH)]
        )
        a_b, cols, cum_t = _decay_terms(dt_b, rate, tri)
        cume = _spread_lanes(cols)
        u = dte * x_all[r]
        seg = segc_ref[r, :]
        entry = dict(a=a_b, dte=dte, cols=cols, cum_t=cum_t, ub=u.astype(jnp.bfloat16))
        prev = segc_ref[b * MIX_ROWS - 1 : b * MIX_ROWS, :] if b > 0 else None
        if b > 0:
            entry["e"] = jnp.where(seg == prev, jnp.exp(cume), 0.0)
        if b < blocks - 1:
            last = cume[MIX_ROWS - 1 : MIX_ROWS, :]
            seg_last = segc_ref[(b + 1) * MIX_ROWS - 1 : (b + 1) * MIX_ROWS, :]
            entry["t"] = jnp.where(seg == seg_last, jnp.exp(last - cume), 0.0)
            entry["tub"] = (entry["t"] * u).astype(jnp.bfloat16)
            if b > 0:
                entry["d"] = jnp.where(seg_last == prev, jnp.exp(last), 0.0)
        return entry

    terms = []
    state = None
    for b in range(blocks):
        r = slice(b * MIX_ROWS, (b + 1) * MIX_ROWS)
        entry = entry_of(b)
        if b > 0:
            keep_ref[b - 1] = state
        if b < blocks - 1:
            fresh = _dot(bt_ref[:, r], entry["tub"])
            state = state * entry["d"] + fresh if b > 0 else fresh
        terms.append(entry if blocks <= 4 else None)

    skip_row = jnp.zeros((1, LANES), jnp.float32)
    gain_row = jnp.zeros((1, LANES), jnp.float32)
    bias_head = jnp.zeros((1, TILEH), jnp.float32)
    rate_head = jnp.zeros((1, TILEH), jnp.float32)
    dst = None
    for b in reversed(range(blocks)):
        r = slice(b * MIX_ROWS, (b + 1) * MIX_ROWS)
        tm = terms[b] or entry_of(b)
        x = x_all[r]
        ub = tm["ub"]
        gate = gate_ref[r, :]
        sg = jax.nn.sigmoid(gate)
        silu = gate * sg
        mixed = mixed_ref[r, :]
        gated = mixed * silu
        dn = dnorm_ref[r, :] * gs_ref[r, :]
        dg = dn * gain - gated * coef_ref[r, :]
        gain_row = gain_row + jnp.sum(dn * gated, axis=0, keepdims=True)
        dgate_ref[r, :] = (dg * mixed * (sg + silu * (1.0 - sg))).astype(jnp.bfloat16)
        dm = dg * silu
        dyb = dm.astype(jnp.bfloat16)
        skip_row = skip_row + jnp.sum(dm * x, axis=0, keepdims=True)
        du = jnp.zeros((MIX_ROWS, LANES), jnp.float32)
        dst_sum = jnp.zeros((MIX_ROWS, MIX_ROWS), jnp.float32)
        for h in range(TILEH):
            wide = jnp.concatenate([tm["cols"][h], tm["cols"][h]], axis=1)
            lt = jnp.exp(jnp.minimum(tm["cum_t"][h : h + 1, :] - wide, 0.0))
            wt = (lt * st_ref[b]).astype(jnp.bfloat16)
            dyh = jnp.where(masks[h], dyb, jnp.zeros_like(dyb))
            du = du + _dot(wt, dyh)
            dst_sum = dst_sum + lt * _dot_t(ub, dyh)
        dst_acc[b] += dst_sum
        ubf = ub.astype(jnp.float32)
        tail = None
        if b < blocks - 1:
            dstb = dst.astype(jnp.bfloat16)
            duf = tm["t"] * _dot(bc_ref[r, 0:STATE], dstb)
            dbc_acc[r, 0:STATE] += _dot_t(tm["tub"], dstb)
            tail = jnp.sum(ubf * duf, axis=0, keepdims=True)
            if b > 0:
                tail = tail + jnp.sum(dst * keep_ref[b - 1], axis=0, keepdims=True) * tm["d"]
            du = du + duf
        y = mixed - x * skip
        z = dyb.astype(jnp.float32) * y - ubf * du
        if tail is not None:
            z = z + jnp.where(_iota((MIX_ROWS, 1), 0) == MIX_ROWS - 1, tail, 0.0)
        if b > 0:
            edy = (tm["e"] * dm).astype(jnp.bfloat16)
            dbc_acc[r, STATE : 2 * STATE] += _dot_t(edy, keep_ref[b - 1].astype(jnp.bfloat16))
            step = _dot(ct_ref[:, r], edy)
            if b < blocks - 1:
                dst = dst * tm["d"] + step
            else:
                dst = step
        c = _dot(tri_up, _split3(per_head(z)))
        da = c[:, 0:TILEH] + c[:, TILEH : 2 * TILEH] + c[:, 2 * TILEH : 3 * TILEH]
        ddt = per_head(du * x) - da * rate
        dsr = ddt * sig_ref[0, r, :]
        dstep_ref[0, r, :] = dsr
        bias_head = bias_head + jnp.sum(dsr, axis=0, keepdims=True)
        rate_head = rate_head + jnp.sum(da * tm["a"], axis=0, keepdims=True)
        s_b = sg_x[r]
        dpre_ref[r, :] = (tm["dte"] * du + skip * dm) * (s_b + x * (1.0 - s_b))

    def conv_back(dpre, v, w):
        out = w[0:1, :] * dpre
        sums = [jnp.sum(dpre * v, axis=0, keepdims=True)]
        for k in range(1, KCONV):
            held = jnp.where(pos >= k, dpre, 0.0)
            out = out + w[k : k + 1, :] * pltpu.roll(held, rows - k, 0)
            sums.append(jnp.sum(held * pltpu.roll(v, k, 0), axis=0, keepdims=True))
        sums.append(jnp.sum(dpre, axis=0, keepdims=True))
        return out, sums

    din, sums = conv_back(dpre_ref[...], inner, cw_ref[...])
    dinner_ref[...] = din.astype(jnp.bfloat16)
    rowsum_ref[...] = jnp.concatenate(
        sums + [gain_row, skip_row, jnp.zeros((1, LANES), jnp.float32)], axis=0
    )
    headsum_ref[0] = jnp.concatenate([bias_head, rate_head], axis=0)

    @pl.when(g == pl.num_programs(1) - 1)
    def _():
        up = _iota((MIX_ROWS, MIX_ROWS), 0) <= _iota((MIX_ROWS, MIX_ROWS), 1)
        for b in range(blocks):
            r = slice(b * MIX_ROWS, (b + 1) * MIX_ROWS)
            ok = (segc_ref[r, :] == segr_ref[:, r]) & up
            ds = jnp.where(ok, dst_acc[b], 0.0).astype(jnp.bfloat16)
            dbc_acc[r, 0:STATE] += _dot(ds, bc_ref[r, STATE : 2 * STATE])
            dbc_acc[r, STATE : 2 * STATE] += _dot_tl(ds, bc_ref[r, 0:STATE])
        sp = state_ref[...]
        pre_s = _conv(sp, csw_ref[...], csb_ref[...], pos)
        sg_s = jax.nn.sigmoid(pre_s)
        dpre_s = dbc_acc[...] * (sg_s + pre_s * sg_s * (1.0 - sg_s))
        dsp, sums_s = conv_back(dpre_s, sp, csw_ref[...])
        dstate_ref[...] = dsp.astype(jnp.bfloat16)
        stsum_ref[...] = jnp.concatenate(
            sums_s + [jnp.zeros((3, 2 * STATE), jnp.float32)], axis=0
        )


def _block(shape, index, single=False):
    if single:
        return pl.BlockSpec(shape, index, pipeline_mode=pl.Buffered(1))
    return pl.BlockSpec(shape, index)


def _tile(rows):
    return _block((rows, LANES), lambda s, g: (s, g), rows > 4 * MIX_ROWS)


def _per_lane(rows):
    return _block((rows, LANES), lambda s, g: (0, g))


def _fixed(shape):
    return _block(shape, lambda s, g: (0,) * len(shape))


def _rows(rows, width):
    return _block((rows, width), lambda s, g: (s, 0), rows > 4 * MIX_ROWS)


def _line(rows):
    return _block((1, rows), lambda s, g: (0, s))


def _heads(rows):
    return _block((1, rows, TILEH), lambda s, g: (g, s, 0), rows > 4 * MIX_ROWS)


def _rate():
    return _block((1, 1, TILEH), lambda s, g: (g, 0, 0))


def mixer_consts(conv_w, conv_b, csw, csb, skip, decay_log, segment, position):
    f = jnp.float32
    head_count = skip.shape[0]
    return dict(
        rate=jnp.exp(decay_log.astype(f)).reshape(head_count // TILEH, 1, TILEH),
        cw=conv_w.astype(f), cb=conv_b.astype(f)[None, :], csw=csw.astype(f), csb=csb.astype(f)[None, :],
        skip=jnp.repeat(skip.astype(f), HEADW)[None, :],
        segc=segment[:, None], segr=segment[None, :], posc=position[:, None],
    )


def mixer_forward(gate, inner, state, dt, k, rows):
    total, width = inner.shape
    blocks = rows // MIX_ROWS
    f = jnp.float32
    wide = jax.ShapeDtypeStruct((total, width), f)
    return pl.pallas_call(
        mixer_fwd_kernel,
        grid=(total // rows, width // LANES),
        in_specs=[
            _tile(rows), _tile(rows), _rows(rows, 2 * STATE), _heads(rows), _rate(),
            _per_lane(KCONV), _per_lane(1), _fixed((KCONV, 2 * STATE)), _fixed((1, 2 * STATE)), _per_lane(1),
            _rows(rows, 1), _line(rows), _rows(rows, 1),
        ],
        out_specs=[_tile(rows), _tile(rows), _rows(rows, 1)],
        out_shape=[wide, wide, jax.ShapeDtypeStruct((total, 1), f)],
        scratch_shapes=[
            pltpu.VMEM((rows, 2 * STATE), jnp.bfloat16),
            pltpu.VMEM((STATE, rows), jnp.bfloat16),
            pltpu.VMEM((blocks, MIX_ROWS, MIX_ROWS), f),
        ],
        cost_estimate=pl.CostEstimate(flops=total * width * 3000, bytes_accessed=total * width * 16, transcendentals=total * width * 6),
        name="mixer_forward",
    )(gate, inner, state, dt, k["rate"], k["cw"], k["cb"], k["csw"], k["csb"], k["skip"],
      k["segc"], k["segr"], k["posc"])


def mixer_backward(gate, inner, mixed, dnorm, gs, coef, gain, state, dt, sig, k, rows):
    total, width = inner.shape
    blocks = rows // MIX_ROWS
    tiles = width // LANES
    spans = total // rows
    f = jnp.float32
    wide = jax.ShapeDtypeStruct((total, width), jnp.bfloat16)
    return pl.pallas_call(
        mixer_bwd_kernel,
        grid=(spans, tiles),
        in_specs=[
            _tile(rows), _tile(rows), _tile(rows), _tile(rows), _rows(rows, 1), _rows(rows, 1), _per_lane(1),
            _rows(rows, 2 * STATE), _heads(rows), _heads(rows), _rate(),
            _per_lane(KCONV), _per_lane(1), _fixed((KCONV, 2 * STATE)), _fixed((1, 2 * STATE)), _per_lane(1),
            _rows(rows, 1), _line(rows), _rows(rows, 1),
        ],
        out_specs=[
            _tile(rows), _tile(rows), _heads(rows), _rows(rows, 2 * STATE),
            _block((8, LANES), lambda s, g: (s, g)),
            _block((1, 2, TILEH), lambda s, g: (s * tiles + g, 0, 0)),
            _block((8, 2 * STATE), lambda s, g: (s, 0)),
        ],
        out_shape=[
            wide, wide, jax.ShapeDtypeStruct((tiles, total, TILEH), f),
            jax.ShapeDtypeStruct((total, 2 * STATE), jnp.bfloat16),
            jax.ShapeDtypeStruct((spans * 8, width), f), jax.ShapeDtypeStruct((spans * tiles, 2, TILEH), f),
            jax.ShapeDtypeStruct((spans * 8, 2 * STATE), f),
        ],
        scratch_shapes=[
            pltpu.VMEM((rows, 2 * STATE), jnp.bfloat16),
            pltpu.VMEM((STATE, rows), jnp.bfloat16),
            pltpu.VMEM((STATE, rows), jnp.bfloat16),
            pltpu.VMEM((blocks, MIX_ROWS, MIX_ROWS), f),
            pltpu.VMEM((blocks, MIX_ROWS, MIX_ROWS), f),
            pltpu.VMEM((rows, 2 * STATE), f),
            pltpu.VMEM((rows, LANES), f),
            pltpu.VMEM((max(blocks - 1, 1), STATE, LANES), f),
        ],
        cost_estimate=pl.CostEstimate(flops=total * width * 6000, bytes_accessed=total * width * 20, transcendentals=total * width * 10),
        name="mixer_backward",
    )(gate, inner, mixed, dnorm, gs, coef, gain, state, dt, sig, k["rate"], k["cw"], k["cb"], k["csw"], k["csb"], k["skip"],
      k["segc"], k["segr"], k["posc"])


def shampoo(weight, gradient, stat_pair, root_pair):
    row_count, col_count = gradient.shape
    blocks = gradient.reshape(row_count // BLK, BLK, col_count // BLK, BLK).transpose(0, 2, 1, 3)
    left_stat = jnp.einsum("abij,abkj->abik", blocks, blocks, precision=HIGHEST)
    right_stat = jnp.einsum("abji,abjk->abik", blocks, blocks, precision=HIGHEST)
    fresh_stats = jnp.stack([left_stat, right_stat], axis=2)
    new_stats = DECAY_RATE * stat_pair + (1.0 - DECAY_RATE) * fresh_stats
    turned = jnp.einsum("abij,abjk->abik", root_pair[:, :, 0], blocks, precision=HIGHEST)
    turned = jnp.einsum("abij,abjk->abik", turned, root_pair[:, :, 1], precision=HIGHEST)
    update_step = turned.transpose(0, 2, 1, 3).reshape(row_count, col_count)
    master = weight - LEARN_RATE * update_step
    return (new_stats, master, master.astype(jnp.bfloat16))


def contract_rows(left_side, right_side):
    return lax.dot_general(
        left_side, right_side, (((0,), (0,)), ((), ())), preferred_element_type=jnp.float32
    )


def contract_cols(left_side, right_side):
    return lax.dot_general(
        left_side, right_side, (((1,), (1,)), ((), ())), preferred_element_type=jnp.float32
    )


Z_RING = 4
CORES = 2


def rank_matrix(keys):
    count = keys.shape[0]
    rank = jnp.sum((keys[None, :] < keys[:, None]).astype(jnp.int32), axis=1)
    return (jnp.arange(count, dtype=jnp.int32)[:, None] == rank[None, :]).astype(jnp.bfloat16)


def move_rows(choose, values):
    return jnp.dot(choose, values, preferred_element_type=jnp.float32).astype(jnp.bfloat16)


def move_back(choose, values):
    return lax.dot_general(
        choose, values, (((0,), (0,)), ((), ())), preferred_element_type=jnp.float32
    ).astype(jnp.bfloat16)


def place_on():
    groups = lax.axis_size("dp")
    ny = groups // (Z_RING * CORES)
    me = lax.axis_index("dp")
    return me // (ny * CORES), (me // CORES) % ny, me % CORES, ny


def shift(values, dz=0, dy=0, dc=0):
    groups = lax.axis_size("dp")
    ny = groups // (Z_RING * CORES)
    pairs = []
    for source in range(groups):
        z, y, c = source // (ny * CORES), (source // CORES) % ny, source % CORES
        pairs.append((source, (((z + dz) % Z_RING) * ny + (y + dy) % ny) * CORES + (c + dc) % CORES))
    return lax.ppermute(values, "dp", pairs)


def swap_dp(values, distance):
    groups = lax.axis_size("dp")
    return lax.ppermute(values, "dp", [(s, s ^ distance) for s in range(groups)])


def swap_tensor(values, distance):
    ranks = lax.axis_size("tensor")
    return lax.ppermute(values, "tensor", [(s, s ^ distance) for s in range(ranks)])


def sum_tensor(values):
    distance = 1
    while distance < lax.axis_size("tensor"):
        values = values + swap_tensor(values, distance)
        distance *= 2
    return values


def flip_halves(values, axis):
    first, second = jnp.split(values, 2, axis=axis)
    return jnp.concatenate([second, first], axis=axis)


def by_core(core, own, other, axis):
    return jnp.where(
        core == 0, jnp.concatenate([own, other], axis=axis), jnp.concatenate([other, own], axis=axis)
    )


def half_of(values, which, axis):
    size = values.shape[axis] // CORES
    return lax.dynamic_slice_in_dim(values, which * size, size, axis)


def gather_weight(weight, name):
    z, y, core, ny = place_on()
    with jax.named_scope(name + "_core"):
        got = shift(half_of(weight, 1 - core, 1), dc=1)
    piece = by_core(core, half_of(weight, core, 1), got, 0)
    rows, width = piece.shape
    full = jnp.zeros((Z_RING * ny * rows, width), weight.dtype)

    def put(full, part, dz, dy):
        at = ((z - dz) % Z_RING * ny + (y - dy) % ny) * rows
        return lax.dynamic_update_slice_in_dim(full, part, at, 0)

    for dz in range(Z_RING):
        full = put(full, piece, dz, 0)
        for dy in range(1, ny):
            with jax.named_scope(f"{name}_y{dz}"):
                across = shift(piece, dy=dy)
            full = put(full, across, dz, dy)
        if dz < Z_RING - 1:
            with jax.named_scope(f"{name}_z{dz}"):
                piece = shift(piece, dz=1)
    return full


def reduce_weight(partial, name):
    z, y, core, ny = place_on()
    rows = partial.shape[0] // (Z_RING * ny)
    f = jnp.float32

    def part(dz, dy):
        at = ((z - dz) % Z_RING * ny + (y + dy) % ny) * rows
        return lax.dynamic_slice_in_dim(partial, at, rows, 0)

    run = None
    for dz in range(1, Z_RING + 1):
        own = part(dz, 0).astype(f)
        for dy in range(1, ny):
            with jax.named_scope(f"{name}_y{dz}"):
                own = own + shift(part(dz, dy), dy=dy).astype(f)
        if run is None:
            run = own
        else:
            with jax.named_scope(f"{name}_z{dz}"):
                run = shift(run.astype(jnp.bfloat16), dz=1).astype(f) + own
    with jax.named_scope(name + "_core"):
        got = shift(half_of(run, 1 - core, 0).astype(jnp.bfloat16), dc=1).astype(f)
    return by_core(core, half_of(run, core, 0), got, 1)


def body(
    tokens, cotangent, norm_gain, w_gate, w_input, w_state, w_step, conv_weight, conv_bias,
    conv_state_weight, conv_state_bias, step_bias, decay_log, skip_gain, gate_gain, w_out,
    stats_gate, stats_input, stats_state, stats_out, roots_gate, roots_input, roots_state, roots_out,
    seq_lens, balance_perm, inverse_perm,
):
    f = jnp.float32
    groups = lax.axis_size("dp")
    tensor_ranks = lax.axis_size("tensor")
    z, y, core, ny = place_on()
    local_rows = tokens.shape[0]
    slot_rows = local_rows // groups
    group_rows = local_rows * tensor_ranks
    heads = step_bias.shape[0] // CORES
    width = w_gate.shape[1] // CORES

    tokens_f = tokens.astype(f)
    scale_in = lax.rsqrt(jnp.mean(tokens_f * tokens_f, axis=1) + EPSILON)
    gain_in = norm_gain.astype(f)
    normed = (tokens_f * scale_in[:, None] * gain_in[None, :]).astype(jnp.bfloat16)
    send_choose = rank_matrix(inverse_perm)

    gate_w = gather_weight(w_gate, "ag_gate")
    input_w = gather_weight(w_input, "ag_input")
    out_w = gather_weight(w_out, "ag_out")
    state_w = lax.all_gather(w_state, "dp", axis=0, tiled=True)
    step_w = half_of(lax.all_gather(w_step, "dp", axis=0, tiled=True), core, 1)

    source = balance_perm // local_rows
    row_key = (source % tensor_ranks * groups + source // tensor_ranks) * group_rows + jnp.arange(
        group_rows, dtype=jnp.int32
    )
    place = rank_matrix(row_key)

    def dispatch(values):
        sent = move_rows(send_choose, values).reshape(groups, slot_rows, D)
        arrived = lax.all_to_all(sent, "dp", split_axis=0, concat_axis=0, tiled=True).reshape(local_rows, D)
        if tensor_ranks == 2:
            rank = lax.axis_index("tensor")
            got = swap_tensor(arrived, 1)
            both = by_core(rank, arrived, got, 0)
        else:
            both = lax.all_gather(arrived, "tensor", axis=0, tiled=True)
        own = move_back(place, both)
        return jnp.concatenate([own, shift(own, dc=1)], axis=0)

    normed_bal = dispatch(normed)
    cot_bal = dispatch(cotangent)

    lens = jnp.concatenate([seq_lens, shift(seq_lens, dc=1)], axis=0)
    first = segment_info(lens[0], group_rows)
    second = segment_info(lens[1], group_rows)
    segment = jnp.concatenate([first[0], second[0]])
    position = jnp.concatenate([first[1], second[1]])

    d_normal = jnp.dot(cot_bal, out_w, preferred_element_type=f)
    gate_proj = jnp.dot(normed_bal, gate_w, preferred_element_type=f)
    inner_proj = jnp.dot(normed_bal, input_w, preferred_element_type=f)
    state_proj = jnp.dot(normed_bal, state_w, preferred_element_type=f)
    step_full = jnp.dot(normed_bal, step_w, preferred_element_type=f)
    step_full = step_full + half_of(step_bias, core, 0).astype(f)[None, :]
    tiles = heads // TILEH
    step_tiles = step_full.reshape(CORES * group_rows, tiles, TILEH).transpose(1, 0, 2)
    step_len = jax.nn.softplus(step_tiles)
    step_slope = jax.nn.sigmoid(step_tiles)
    consts = mixer_consts(
        half_of(conv_weight, core, 1), half_of(conv_bias, core, 0), conv_state_weight, conv_state_bias,
        half_of(skip_gain, core, 0), half_of(decay_log, core, 0), segment, position,
    )
    gain_gate = half_of(gate_gain, core, 0).astype(f)
    mixed, gated_out, square = mixer_forward(gate_proj, inner_proj, state_proj, step_len, consts, group_rows)
    inner_dot = jnp.sum(gated_out * gain_gate[None, :] * d_normal, axis=1)
    row_stats = jnp.stack([square[:, 0], inner_dot])
    row_stats = row_stats + flip_halves(shift(row_stats, dc=1), 1)
    row_stats = sum_tensor(row_stats)
    gate_scale = lax.rsqrt(row_stats[0] / INNER + EPSILON)
    coef = gate_scale**3 * row_stats[1] / INNER
    normal = (gated_out * gate_scale[:, None] * gain_gate[None, :]).astype(jnp.bfloat16)

    d_gate, d_inner, d_step, d_state, row_sums, head_sums, state_sums = mixer_backward(
        gate_proj, inner_proj, mixed, d_normal, gate_scale[:, None], coef[:, None], gain_gate[None, :],
        state_proj, step_len, step_slope, consts, group_rows,
    )
    d_step = d_step.transpose(1, 0, 2).reshape(CORES * group_rows, heads).astype(jnp.bfloat16)

    out_grad = reduce_weight(contract_rows(cot_bal, normal).astype(jnp.bfloat16), "rs_out")
    gate_grad = reduce_weight(contract_rows(normed_bal, d_gate).astype(jnp.bfloat16), "rs_gate")
    input_grad = reduce_weight(contract_rows(normed_bal, d_inner).astype(jnp.bfloat16), "rs_input")

    def give_back(partial):
        own, other = jnp.split(partial, 2, axis=0)
        own = (own.astype(f) + shift(other, dc=1).astype(f)).astype(jnp.bfloat16)
        arranged = move_rows(place, own)
        if tensor_ranks == 2:
            rank = lax.axis_index("tensor")
            mine = half_of(arranged, rank, 0).astype(f)
            total = (mine + swap_tensor(half_of(arranged, 1 - rank, 0), 1).astype(f)).astype(jnp.bfloat16)
        else:
            total = lax.psum_scatter(arranged, "tensor", scatter_dimension=0, tiled=True)
        returned = lax.all_to_all(
            total.reshape(groups, slot_rows, D), "dp", split_axis=0, concat_axis=0, tiled=True
        )
        return move_back(send_choose, returned.reshape(local_rows, D)).astype(f)

    branch = give_back(contract_cols(normal, out_w).astype(jnp.bfloat16))
    column_term = (
        contract_cols(d_gate, gate_w)
        + contract_cols(d_inner, input_w)
        + contract_cols(d_state, state_w)
        + contract_cols(d_step, step_w)
    )
    norm_gain_part = jnp.sum(column_term * normed_bal.astype(f), axis=0) / gain_in
    d_tokens_normed = give_back(column_term.astype(jnp.bfloat16))

    state_part = contract_rows(normed_bal, d_state).astype(jnp.bfloat16)
    step_part = contract_rows(normed_bal, d_step).astype(jnp.bfloat16)
    step_part = jnp.where(
        (jnp.arange(CORES * heads, dtype=jnp.int32) // heads == core)[None, :],
        jnp.concatenate([step_part] * CORES, axis=1),
        jnp.zeros((), jnp.bfloat16),
    )
    thin = lax.psum_scatter(
        jnp.concatenate([state_part, step_part], axis=1), "dp", scatter_dimension=0, tiled=True
    )
    state_grad = sum_tensor(thin[:, : 2 * STATE].astype(f))
    step_grad = thin[:, 2 * STATE :].astype(f)

    row_sums = jnp.sum(row_sums.reshape(CORES, 8, width), axis=0)
    head_sums = jnp.sum(head_sums.reshape(CORES, tiles, 2, TILEH), axis=0).transpose(1, 0, 2).reshape(2, heads)
    skip_sums = jnp.sum(row_sums[KCONV + 2].reshape(heads, HEADW), axis=1)
    state_sums = jnp.sum(state_sums.reshape(CORES, 8, 2 * STATE), axis=0)[: KCONV + 1]
    split_part = jnp.concatenate([row_sums[: KCONV + 2].reshape(-1), head_sums.reshape(-1), skip_sums])
    shared_part = jnp.concatenate([norm_gain_part, state_sums.reshape(-1)])
    packed = jnp.concatenate([split_part, shared_part])
    distance = CORES
    while distance < groups:
        packed = packed + swap_dp(packed, distance)
        distance *= 2
    partner = shift(packed, dc=1)
    edge = split_part.shape[0]
    shared = sum_tensor(packed[edge:] + partner[edge:])
    lanes = (KCONV + 2) * width
    wide_sums = by_core(
        core, packed[:lanes].reshape(KCONV + 2, width), partner[:lanes].reshape(KCONV + 2, width), 1
    )
    thin_sums = by_core(
        core, packed[lanes:edge].reshape(3, heads), partner[lanes:edge].reshape(3, heads), 1
    )
    norm_gain_grad = shared[:D]
    conv_state_grads = shared[D:].reshape(KCONV + 1, 2 * STATE)

    block_out = tokens_f + branch
    dot_in = jnp.sum(tokens_f * gain_in[None, :] * d_tokens_normed, axis=1)
    tokens_grad = (
        cotangent.astype(f)
        + d_tokens_normed * scale_in[:, None] * gain_in[None, :]
        - tokens_f * (scale_in**3 * dot_in / D)[:, None]
    )
    new_gate = shampoo(w_gate.astype(f), gate_grad, stats_gate, roots_gate)
    new_input = shampoo(w_input.astype(f), input_grad, stats_input, roots_input)
    new_state = shampoo(w_state.astype(f), state_grad, stats_state, roots_state)
    new_out = shampoo(w_out.astype(f), out_grad, stats_out, roots_out)
    return (
        block_out, tokens_grad, norm_gain_grad, gate_grad, input_grad, state_grad, step_grad,
        wide_sums[:KCONV], wide_sums[KCONV], conv_state_grads[:KCONV], conv_state_grads[KCONV],
        thin_sums[0], thin_sums[1], thin_sums[2], wide_sums[KCONV + 1], out_grad,
        new_gate[0], new_input[0], new_state[0], new_out[0],
        new_gate[1], new_input[1], new_state[1], new_out[1],
        new_gate[2], new_input[2], new_state[2], new_out[2],
    )


def solution(mesh):
    placed = (
        P(("dp", "tensor"), None),
        P(("dp", "tensor"), None),
        P(),
        P("dp", "tensor"),
        P("dp", "tensor"),
        P("dp", None),
        P("dp", "tensor"),
        P(None, "tensor"),
        P("tensor"),
        P(),
        P(),
        P("tensor"),
        P("tensor"),
        P("tensor"),
        P("tensor"),
        P("dp", "tensor"),
        P("dp", "tensor", None, None, None),
        P("dp", "tensor", None, None, None),
        P("dp", None, None, None, None),
        P("dp", "tensor", None, None, None),
        P("dp", "tensor", None, None, None),
        P("dp", "tensor", None, None, None),
        P("dp", None, None, None, None),
        P("dp", "tensor", None, None, None),
        P("dp", None),
        P("dp"),
        P(("dp", "tensor")),
    )
    return jax.shard_map(
        body,
        mesh=mesh,
        in_specs=placed,
        out_specs=(
            P(("dp", "tensor"), None),
            P(("dp", "tensor"), None),
            P(),
            P("dp", "tensor"),
            P("dp", "tensor"),
            P("dp", None),
            P("dp", "tensor"),
            P(None, "tensor"),
            P("tensor"),
            P(),
            P(),
            P("tensor"),
            P("tensor"),
            P("tensor"),
            P("tensor"),
            P("dp", "tensor"),
            P("dp", "tensor", None, None, None),
            P("dp", "tensor", None, None, None),
            P("dp", None, None, None, None),
            P("dp", "tensor", None, None, None),
            P("dp", "tensor"),
            P("dp", "tensor"),
            P("dp", None),
            P("dp", "tensor"),
            P("dp", "tensor"),
            P("dp", "tensor"),
            P("dp", None),
            P("dp", "tensor"),
        ),
        check_vma=False,
    )
```

```python
import jax
import jax.numpy as jnp
from jax import lax
from jax.experimental import pallas as pl
from jax.experimental.pallas import tpu as pltpu
from jax.sharding import PartitionSpec as P


D = 2048
STATE = 128
KCONV = 4
BLK = 64
INNER = 4096


EPSILON = 1e-05
DECAY_RATE = 0.5
LEARN_RATE = 0.2


def segment_info(lengths, row_count):
    starts = jnp.cumsum(lengths) - lengths
    row_index = jnp.arange(row_count, dtype=jnp.int32)
    passed = row_index[:, None] >= starts[None, :]
    segment = jnp.sum(passed.astype(jnp.int32), axis=1) - 1
    seq_begin = jnp.max(jnp.where(passed, starts[None, :], 0), axis=1)
    return (segment, row_index - seq_begin)


MIX_ROWS = 256
LANES = 256
HEADW = 64
TILEH = LANES // HEADW


def _split3(v):
    hi = v.astype(jnp.bfloat16)
    r1 = v - hi.astype(jnp.float32)
    mid = r1.astype(jnp.bfloat16)
    lo = (r1 - mid.astype(jnp.float32)).astype(jnp.bfloat16)
    return jnp.concatenate([hi, mid, lo], axis=1)


def _dot(a, b):
    return lax.dot_general(a, b, (((1,), (0,)), ((), ())), preferred_element_type=jnp.float32)


def _dot_t(a, b):
    return lax.dot_general(a, b, (((1,), (1,)), ((), ())), preferred_element_type=jnp.float32)


def _dot_tl(a, b):
    return lax.dot_general(a, b, (((0,), (0,)), ((), ())), preferred_element_type=jnp.float32)


def _conv(v, w, b, pos):
    out = w[0:1, :] * v + b
    for k in range(1, KCONV):
        out = out + jnp.where(pos >= k, pltpu.roll(v, k, 0), 0.0) * w[k : k + 1, :]
    return out


def _iota(shape, axis):
    return lax.broadcasted_iota(jnp.int32, shape, axis)


def _lower():
    return _iota((MIX_ROWS, MIX_ROWS), 0) >= _iota((MIX_ROWS, MIX_ROWS), 1)


def _head_masks():
    lane = _iota((1, LANES), 1) // HEADW
    return [(lane == h) for h in range(TILEH)]


def _spread_lanes(cols):
    lane = _iota((1, 2 * HEADW), 1)
    return jnp.concatenate(
        [jnp.where(lane < HEADW, cols[2 * i], cols[2 * i + 1]) for i in range(TILEH // 2)], axis=1
    )


def _decay_terms(dt_b, rate, tri):
    a_b = -dt_b * rate
    parts = _split3(a_b)
    c = _dot(tri, parts)
    cum = c[:, 0:TILEH] + c[:, TILEH : 2 * TILEH] + c[:, 2 * TILEH : 3 * TILEH]
    ct = lax.dot_general(parts, tri, (((0,), (1,)), ((), ())), preferred_element_type=jnp.float32)
    cum_t = ct[0:TILEH] + ct[TILEH : 2 * TILEH] + ct[2 * TILEH : 3 * TILEH]
    cols = [jnp.broadcast_to(cum[:, h : h + 1], (MIX_ROWS, 128)) for h in range(TILEH)]
    return a_b, cols, cum_t


def mixer_fwd_kernel(
    gate_ref, inner_ref, state_ref, dt_ref, rate_ref, cw_ref, cb_ref, csw_ref, csb_ref, skip_ref,
    segc_ref, segr_ref, posc_ref,
    mixed_ref, gated_ref, square_ref,
    bc_ref, bt_ref, s_ref,
):
    rows = inner_ref.shape[0]
    blocks = rows // MIX_ROWS
    pos = posc_ref[...]
    g = pl.program_id(1)

    @pl.when(g == 0)
    def _():
        pre = _conv(state_ref[...], csw_ref[...], csb_ref[...], pos)
        act = pre * jax.nn.sigmoid(pre)
        bc_ref[...] = act.astype(jnp.bfloat16)
        low = _lower()
        for b in range(blocks):
            r = slice(b * MIX_ROWS, (b + 1) * MIX_ROWS)
            bt_ref[:, r] = jnp.transpose(act[r, 0:STATE]).astype(jnp.bfloat16)
            s = _dot_t(bc_ref[r, STATE : 2 * STATE], bc_ref[r, 0:STATE])
            ok = (segc_ref[r, :] == segr_ref[:, r]) & low
            s_ref[b] = jnp.where(ok, s, 0.0)
        square_ref[...] = jnp.zeros_like(square_ref)

    pre = _conv(inner_ref[...], cw_ref[...], cb_ref[...], pos)
    x_all = pre * jax.nn.sigmoid(pre)
    tri = jnp.where(_lower(), 1.0, 0.0).astype(jnp.bfloat16)
    masks = _head_masks()
    rate = rate_ref[0]
    skip = skip_ref[...]
    state = jnp.zeros((STATE, LANES), jnp.float32)
    for b in range(blocks):
        r = slice(b * MIX_ROWS, (b + 1) * MIX_ROWS)
        dt_b = dt_ref[0, r, :]
        x = x_all[r]
        dte = _spread_lanes(
            [jnp.broadcast_to(dt_b[:, h : h + 1], (MIX_ROWS, 128)) for h in range(TILEH)]
        )
        u = dte * x
        ub = u.astype(jnp.bfloat16)
        _, cols, cum_t = _decay_terms(dt_b, rate, tri)
        cume = _spread_lanes(cols)
        seg = segc_ref[r, :]
        y = jnp.zeros((MIX_ROWS, LANES), jnp.float32)
        for h in range(TILEH):
            wide = jnp.concatenate([cols[h], cols[h]], axis=1)
            w = jnp.exp(jnp.minimum(wide - cum_t[h : h + 1, :], 0.0)) * s_ref[b]
            y = y + _dot(w.astype(jnp.bfloat16), jnp.where(masks[h], ub, jnp.zeros_like(ub)))
        if b > 0:
            alive = seg == segc_ref[b * MIX_ROWS - 1 : b * MIX_ROWS, :]
            carried = _dot(bc_ref[r, STATE : 2 * STATE], state.astype(jnp.bfloat16))
            y = y + carried * jnp.where(alive, jnp.exp(cume), 0.0)
        if b < blocks - 1:
            last = cume[MIX_ROWS - 1 : MIX_ROWS, :]
            seg_last = segc_ref[(b + 1) * MIX_ROWS - 1 : (b + 1) * MIX_ROWS, :]
            toward = jnp.where(seg == seg_last, jnp.exp(last - cume), 0.0)
            fresh = _dot(bt_ref[:, r], (toward * u).astype(jnp.bfloat16))
            if b > 0:
                keep = seg_last == segc_ref[b * MIX_ROWS - 1 : b * MIX_ROWS, :]
                state = state * jnp.where(keep, jnp.exp(last), 0.0) + fresh
            else:
                state = fresh
        mixed = y + x * skip
        gate = gate_ref[r, :]
        gated = mixed * (gate * jax.nn.sigmoid(gate))
        mixed_ref[r, :] = mixed
        gated_ref[r, :] = gated
        square_ref[r, :] += jnp.sum(gated * gated, axis=1, keepdims=True)


def mixer_bwd_kernel(
    gate_ref, inner_ref, mixed_ref, dnorm_ref, gs_ref, coef_ref, gain_ref,
    state_ref, dt_ref, sig_ref, rate_ref, cw_ref, cb_ref, csw_ref, csb_ref, skip_ref,
    segc_ref, segr_ref, posc_ref,
    dinner_ref, dstep_ref, dstate_ref, rowsum_ref, headsum_ref, stsum_ref,
    bc_ref, bt_ref, ct_ref, st_ref, dst_acc, dbc_acc, dpre_ref, keep_ref,
):
    rows = inner_ref.shape[0]
    blocks = rows // MIX_ROWS
    pos = posc_ref[...]
    g = pl.program_id(1)

    @pl.when(g == 0)
    def _():
        pre = _conv(state_ref[...], csw_ref[...], csb_ref[...], pos)
        act = pre * jax.nn.sigmoid(pre)
        bc_ref[...] = act.astype(jnp.bfloat16)
        up = _iota((MIX_ROWS, MIX_ROWS), 0) <= _iota((MIX_ROWS, MIX_ROWS), 1)
        for b in range(blocks):
            r = slice(b * MIX_ROWS, (b + 1) * MIX_ROWS)
            bt_ref[:, r] = jnp.transpose(act[r, 0:STATE]).astype(jnp.bfloat16)
            ct_ref[:, r] = jnp.transpose(act[r, STATE : 2 * STATE]).astype(jnp.bfloat16)
            s = _dot_t(bc_ref[r, 0:STATE], bc_ref[r, STATE : 2 * STATE])
            ok = (segc_ref[r, :] == segr_ref[:, r]) & up
            st_ref[b] = jnp.where(ok, s, 0.0)
        dst_acc[...] = jnp.zeros_like(dst_acc)
        dbc_acc[...] = jnp.zeros_like(dbc_acc)

    inner = inner_ref[...]
    pre = _conv(inner, cw_ref[...], cb_ref[...], pos)
    sg_x = jax.nn.sigmoid(pre)
    x_all = pre * sg_x
    tri = jnp.where(_lower(), 1.0, 0.0).astype(jnp.bfloat16)
    tri_up = jnp.where(
        _iota((MIX_ROWS, MIX_ROWS), 0) <= _iota((MIX_ROWS, MIX_ROWS), 1), 1.0, 0.0
    ).astype(jnp.bfloat16)
    masks = _head_masks()
    pick = jnp.where(
        _iota((LANES, TILEH), 0) // HEADW == _iota((LANES, TILEH), 1), 1.0, 0.0
    ).astype(jnp.bfloat16)
    rate = rate_ref[0]
    skip = skip_ref[...]
    gain = gain_ref[...]

    def per_head(v):
        hi = v.astype(jnp.bfloat16)
        lo = (v - hi.astype(jnp.float32)).astype(jnp.bfloat16)
        return _dot(hi, pick) + _dot(lo, pick)

    def entry_of(b):
        r = slice(b * MIX_ROWS, (b + 1) * MIX_ROWS)
        dt_b = dt_ref[0, r, :]
        dte = _spread_lanes(
            [jnp.broadcast_to(dt_b[:, h : h + 1], (MIX_ROWS, 128)) for h in range(TILEH)]
        )
        a_b, cols, cum_t = _decay_terms(dt_b, rate, tri)
        cume = _spread_lanes(cols)
        u = dte * x_all[r]
        seg = segc_ref[r, :]
        entry = dict(a=a_b, dte=dte, cols=cols, cum_t=cum_t, ub=u.astype(jnp.bfloat16))
        prev = segc_ref[b * MIX_ROWS - 1 : b * MIX_ROWS, :] if b > 0 else None
        if b > 0:
            entry["e"] = jnp.where(seg == prev, jnp.exp(cume), 0.0)
        if b < blocks - 1:
            last = cume[MIX_ROWS - 1 : MIX_ROWS, :]
            seg_last = segc_ref[(b + 1) * MIX_ROWS - 1 : (b + 1) * MIX_ROWS, :]
            entry["t"] = jnp.where(seg == seg_last, jnp.exp(last - cume), 0.0)
            entry["tub"] = (entry["t"] * u).astype(jnp.bfloat16)
            if b > 0:
                entry["d"] = jnp.where(seg_last == prev, jnp.exp(last), 0.0)
        return entry

    terms = []
    state = None
    for b in range(blocks):
        r = slice(b * MIX_ROWS, (b + 1) * MIX_ROWS)
        entry = entry_of(b)
        if b > 0:
            keep_ref[b - 1] = state
        if b < blocks - 1:
            fresh = _dot(bt_ref[:, r], entry["tub"])
            state = state * entry["d"] + fresh if b > 0 else fresh
        terms.append(entry if blocks <= 4 else None)

    skip_row = jnp.zeros((1, LANES), jnp.float32)
    gain_row = jnp.zeros((1, LANES), jnp.float32)
    bias_head = jnp.zeros((1, TILEH), jnp.float32)
    rate_head = jnp.zeros((1, TILEH), jnp.float32)
    dst = None
    for b in reversed(range(blocks)):
        r = slice(b * MIX_ROWS, (b + 1) * MIX_ROWS)
        tm = terms[b] or entry_of(b)
        x = x_all[r]
        ub = tm["ub"]
        gate = gate_ref[r, :]
        sg = jax.nn.sigmoid(gate)
        silu = gate * sg
        mixed = mixed_ref[r, :]
        gated = mixed * silu
        dn = dnorm_ref[r, :] * gs_ref[r, :]
        dg = dn * gain - gated * coef_ref[r, :]
        gain_row = gain_row + jnp.sum(dn * gated, axis=0, keepdims=True)
        dm = dg * silu
        dyb = dm.astype(jnp.bfloat16)
        skip_row = skip_row + jnp.sum(dm * x, axis=0, keepdims=True)
        du = jnp.zeros((MIX_ROWS, LANES), jnp.float32)
        dst_sum = jnp.zeros((MIX_ROWS, MIX_ROWS), jnp.float32)
        for h in range(TILEH):
            wide = jnp.concatenate([tm["cols"][h], tm["cols"][h]], axis=1)
            lt = jnp.exp(jnp.minimum(tm["cum_t"][h : h + 1, :] - wide, 0.0))
            wt = (lt * st_ref[b]).astype(jnp.bfloat16)
            dyh = jnp.where(masks[h], dyb, jnp.zeros_like(dyb))
            du = du + _dot(wt, dyh)
            dst_sum = dst_sum + lt * _dot_t(ub, dyh)
        dst_acc[b] += dst_sum
        ubf = ub.astype(jnp.float32)
        tail = None
        if b < blocks - 1:
            dstb = dst.astype(jnp.bfloat16)
            duf = tm["t"] * _dot(bc_ref[r, 0:STATE], dstb)
            dbc_acc[r, 0:STATE] += _dot_t(tm["tub"], dstb)
            tail = jnp.sum(ubf * duf, axis=0, keepdims=True)
            if b > 0:
                tail = tail + jnp.sum(dst * keep_ref[b - 1], axis=0, keepdims=True) * tm["d"]
            du = du + duf
        y = mixed - x * skip
        z = dyb.astype(jnp.float32) * y - ubf * du
        if tail is not None:
            z = z + jnp.where(_iota((MIX_ROWS, 1), 0) == MIX_ROWS - 1, tail, 0.0)
        if b > 0:
            edy = (tm["e"] * dm).astype(jnp.bfloat16)
            dbc_acc[r, STATE : 2 * STATE] += _dot_t(edy, keep_ref[b - 1].astype(jnp.bfloat16))
            step = _dot(ct_ref[:, r], edy)
            if b < blocks - 1:
                dst = dst * tm["d"] + step
            else:
                dst = step
        c = _dot(tri_up, _split3(per_head(z)))
        da = c[:, 0:TILEH] + c[:, TILEH : 2 * TILEH] + c[:, 2 * TILEH : 3 * TILEH]
        ddt = per_head(du * x) - da * rate
        dsr = ddt * sig_ref[0, r, :]
        dstep_ref[0, r, :] = dsr
        bias_head = bias_head + jnp.sum(dsr, axis=0, keepdims=True)
        rate_head = rate_head + jnp.sum(da * tm["a"], axis=0, keepdims=True)
        s_b = sg_x[r]
        dpre_ref[r, :] = (tm["dte"] * du + skip * dm) * (s_b + x * (1.0 - s_b))

    def conv_back(dpre, v, w):
        out = w[0:1, :] * dpre
        sums = [jnp.sum(dpre * v, axis=0, keepdims=True)]
        for k in range(1, KCONV):
            held = jnp.where(pos >= k, dpre, 0.0)
            out = out + w[k : k + 1, :] * pltpu.roll(held, rows - k, 0)
            sums.append(jnp.sum(held * pltpu.roll(v, k, 0), axis=0, keepdims=True))
        sums.append(jnp.sum(dpre, axis=0, keepdims=True))
        return out, sums

    din, sums = conv_back(dpre_ref[...], inner, cw_ref[...])
    dinner_ref[...] = din.astype(jnp.bfloat16)
    rowsum_ref[...] = jnp.concatenate(
        sums + [gain_row, skip_row, jnp.zeros((1, LANES), jnp.float32)], axis=0
    )
    headsum_ref[0] = jnp.concatenate([bias_head, rate_head], axis=0)

    @pl.when(g == pl.num_programs(1) - 1)
    def _():
        up = _iota((MIX_ROWS, MIX_ROWS), 0) <= _iota((MIX_ROWS, MIX_ROWS), 1)
        for b in range(blocks):
            r = slice(b * MIX_ROWS, (b + 1) * MIX_ROWS)
            ok = (segc_ref[r, :] == segr_ref[:, r]) & up
            ds = jnp.where(ok, dst_acc[b], 0.0).astype(jnp.bfloat16)
            dbc_acc[r, 0:STATE] += _dot(ds, bc_ref[r, STATE : 2 * STATE])
            dbc_acc[r, STATE : 2 * STATE] += _dot_tl(ds, bc_ref[r, 0:STATE])
        sp = state_ref[...]
        pre_s = _conv(sp, csw_ref[...], csb_ref[...], pos)
        sg_s = jax.nn.sigmoid(pre_s)
        dpre_s = dbc_acc[...] * (sg_s + pre_s * sg_s * (1.0 - sg_s))
        dsp, sums_s = conv_back(dpre_s, sp, csw_ref[...])
        dstate_ref[...] = dsp.astype(jnp.bfloat16)
        stsum_ref[...] = jnp.concatenate(
            sums_s + [jnp.zeros((3, 2 * STATE), jnp.float32)], axis=0
        )


def _block(shape, index, single=False):
    if single:
        return pl.BlockSpec(shape, index, pipeline_mode=pl.Buffered(1))
    return pl.BlockSpec(shape, index)


def _tile(rows, first=0):
    return _block((rows, LANES), lambda s, g: (s + first, g), rows > 4 * MIX_ROWS)


def _per_lane(rows):
    return _block((rows, LANES), lambda s, g: (0, g))


def _fixed(shape):
    return _block(shape, lambda s, g: (0,) * len(shape))


def _rows(rows, width, first=0):
    return _block((rows, width), lambda s, g: (s + first, 0), rows > 4 * MIX_ROWS)


def _state(rows, at, first=0):
    return _block((rows, 2 * STATE), lambda s, g: (s + first, at), rows > 4 * MIX_ROWS)


def _line(rows, first=0):
    return _block((1, rows), lambda s, g: (0, s + first))


def _heads(rows, first=0):
    return _block((1, rows, TILEH), lambda s, g: (g, s + first, 0), rows > 4 * MIX_ROWS)


def _rate():
    return _block((1, 1, TILEH), lambda s, g: (g, 0, 0))


def mixer_consts(conv_w, conv_b, csw, csb, skip, decay_log, segment, position):
    f = jnp.float32
    head_count = skip.shape[0]
    return dict(
        rate=jnp.exp(decay_log.astype(f)).reshape(head_count // TILEH, 1, TILEH),
        cw=conv_w.astype(f), cb=conv_b.astype(f)[None, :], csw=csw.astype(f), csb=csb.astype(f)[None, :],
        skip=jnp.repeat(skip.astype(f), HEADW)[None, :],
        segc=segment[:, None], segr=segment[None, :], posc=position[:, None],
    )


def mixer_forward(gate, joined, dt, k, rows):
    total, width = gate.shape
    at = width // (2 * STATE)
    blocks = rows // MIX_ROWS
    f = jnp.float32
    wide = jax.ShapeDtypeStruct((total, width), f)
    return pl.pallas_call(
        mixer_fwd_kernel,
        grid=(total // rows, width // LANES),
        in_specs=[
            _tile(rows), _tile(rows), _state(rows, at), _heads(rows), _rate(),
            _per_lane(KCONV), _per_lane(1), _fixed((KCONV, 2 * STATE)), _fixed((1, 2 * STATE)), _per_lane(1),
            _rows(rows, 1), _line(rows), _rows(rows, 1),
        ],
        out_specs=[_tile(rows), _tile(rows), _rows(rows, 1)],
        out_shape=[wide, wide, jax.ShapeDtypeStruct((total, 1), f)],
        scratch_shapes=[
            pltpu.VMEM((rows, 2 * STATE), jnp.bfloat16),
            pltpu.VMEM((STATE, rows), jnp.bfloat16),
            pltpu.VMEM((blocks, MIX_ROWS, MIX_ROWS), f),
        ],
        cost_estimate=pl.CostEstimate(flops=total * width * 3000, bytes_accessed=total * width * 16, transcendentals=total * width * 6),
        name="mixer_forward",
    )(gate, joined, joined, dt, k["rate"], k["cw"], k["cb"], k["csw"], k["csb"], k["skip"],
      k["segc"], k["segr"], k["posc"])


def mixer_backward(gate, joined, mixed, dnorm, gs, coef, gain, dt, sig, k, rows, first):
    _, width = gate.shape
    at = width // (2 * STATE)
    blocks = rows // MIX_ROWS
    tiles = width // LANES
    spans = 1
    f = jnp.float32
    wide = jax.ShapeDtypeStruct((rows, width), jnp.bfloat16)
    return pl.pallas_call(
        mixer_bwd_kernel,
        grid=(spans, tiles),
        in_specs=[
            _tile(rows, first), _tile(rows, first), _tile(rows, first), _tile(rows, first),
            _rows(rows, 1, first), _rows(rows, 1, first), _per_lane(1),
            _state(rows, at, first), _heads(rows, first), _heads(rows, first), _rate(),
            _per_lane(KCONV), _per_lane(1), _fixed((KCONV, 2 * STATE)), _fixed((1, 2 * STATE)), _per_lane(1),
            _rows(rows, 1, first), _line(rows, first), _rows(rows, 1, first),
        ],
        out_specs=[
            _tile(rows), _heads(rows), _rows(rows, 2 * STATE),
            _block((8, LANES), lambda s, g: (s, g)),
            _block((1, 2, TILEH), lambda s, g: (s * tiles + g, 0, 0)),
            _block((8, 2 * STATE), lambda s, g: (s, 0)),
        ],
        out_shape=[
            wide, jax.ShapeDtypeStruct((tiles, rows, TILEH), f),
            jax.ShapeDtypeStruct((rows, 2 * STATE), jnp.bfloat16),
            jax.ShapeDtypeStruct((spans * 8, width), f), jax.ShapeDtypeStruct((spans * tiles, 2, TILEH), f),
            jax.ShapeDtypeStruct((spans * 8, 2 * STATE), f),
        ],
        scratch_shapes=[
            pltpu.VMEM((rows, 2 * STATE), jnp.bfloat16),
            pltpu.VMEM((STATE, rows), jnp.bfloat16),
            pltpu.VMEM((STATE, rows), jnp.bfloat16),
            pltpu.VMEM((blocks, MIX_ROWS, MIX_ROWS), f),
            pltpu.VMEM((blocks, MIX_ROWS, MIX_ROWS), f),
            pltpu.VMEM((rows, 2 * STATE), f),
            pltpu.VMEM((rows, LANES), f),
            pltpu.VMEM((max(blocks - 1, 1), STATE, LANES), f),
        ],
        cost_estimate=pl.CostEstimate(flops=rows * width * 6000, bytes_accessed=rows * width * 20, transcendentals=rows * width * 10),
        name="mixer_backward",
    )(gate, joined, mixed, dnorm, gs, coef, gain, joined, dt, sig, k["rate"], k["cw"], k["cb"], k["csw"], k["csb"], k["skip"],
      k["segc"], k["segr"], k["posc"])


def shampoo_kernel(w_ref, g_ref, stats_ref, roots_ref, new_ref, master_ref, copy_ref):
    high, across = stats_ref.shape[0], stats_ref.shape[1]
    span = across * BLK
    lane = lax.broadcasted_iota(jnp.int32, (BLK, span), 1) // BLK
    zero = jnp.zeros((), jnp.bfloat16)
    empty = jnp.zeros((BLK, BLK), jnp.bfloat16)
    for a in range(high):
        rows = slice(a * BLK, (a + 1) * BLK)
        tile = g_ref[rows, :].astype(jnp.bfloat16)
        apart = jnp.concatenate([jnp.where(lane == b, tile, zero) for b in range(across)], axis=0)
        left = _dot_t(apart, tile)
        right = _dot_tl(tile, tile)
        firsts = jnp.concatenate([roots_ref[a, b, 0].astype(jnp.bfloat16) for b in range(across)], axis=0)
        turned = _dot(firsts, tile)
        half = turned[0:BLK]
        for b in range(1, across):
            half = jnp.where(lane == b, turned[b * BLK : (b + 1) * BLK], half)
        joint = jnp.concatenate(
            [
                jnp.concatenate(
                    [roots_ref[a, b, 1].astype(jnp.bfloat16) if c == b else empty for c in range(across)], axis=1
                )
                for b in range(across)
            ],
            axis=0,
        )
        step = _dot(half.astype(jnp.bfloat16), joint)
        for b in range(across):
            part = slice(b * BLK, (b + 1) * BLK)
            new_ref[a, b, 0] = DECAY_RATE * stats_ref[a, b, 0] + (1.0 - DECAY_RATE) * left[part, :]
            new_ref[a, b, 1] = DECAY_RATE * stats_ref[a, b, 1] + (1.0 - DECAY_RATE) * right[part, part]
        master = w_ref[rows, :].astype(jnp.float32) - LEARN_RATE * step
        master_ref[rows, :] = master
        copy_ref[rows, :] = master.astype(jnp.bfloat16)


def shampoo(weight, gradient, stat_pair, root_pair):
    rows, cols = gradient.shape
    step = min(cols, 256)
    plain = pl.BlockSpec((rows, step), lambda i: (0, i))
    pairs = pl.BlockSpec((rows // BLK, step // BLK, 2, BLK, BLK), lambda i: (0, i, 0, 0, 0))
    return pl.pallas_call(
        shampoo_kernel,
        grid=(cols // step,),
        in_specs=[plain, plain, pairs, pairs],
        out_specs=[pairs, plain, plain],
        out_shape=[
            jax.ShapeDtypeStruct(stat_pair.shape, jnp.float32),
            jax.ShapeDtypeStruct((rows, cols), jnp.float32),
            jax.ShapeDtypeStruct((rows, cols), jnp.bfloat16),
        ],
        cost_estimate=pl.CostEstimate(flops=rows * cols * 512, bytes_accessed=rows * cols * 40, transcendentals=0),
        compiler_params=pltpu.CompilerParams(vmem_limit_bytes=24 * 2**20),
        name="shampoo",
    )(weight, gradient, stat_pair, root_pair)


def contract_rows(left_side, right_side):
    return lax.dot_general(
        left_side, right_side, (((0,), (0,)), ((), ())), preferred_element_type=jnp.float32
    )


def contract_cols(left_side, right_side):
    return lax.dot_general(
        left_side, right_side, (((1,), (1,)), ((), ())), preferred_element_type=jnp.float32
    )


Z_RING = 4
CORES = 2


def rank_matrix(keys):
    count = keys.shape[0]
    rank = jnp.sum((keys[None, :] < keys[:, None]).astype(jnp.int32), axis=1)
    return (jnp.arange(count, dtype=jnp.int32)[:, None] == rank[None, :]).astype(jnp.bfloat16)


def move_rows(choose, values):
    return jnp.dot(choose, values, preferred_element_type=jnp.float32).astype(jnp.bfloat16)


def move_back(choose, values):
    return lax.dot_general(
        choose, values, (((0,), (0,)), ((), ())), preferred_element_type=jnp.float32
    ).astype(jnp.bfloat16)


def place_on():
    groups = lax.axis_size("dp")
    ny = groups // (Z_RING * CORES)
    me = lax.axis_index("dp")
    return me // (ny * CORES), (me // CORES) % ny, me % CORES, ny


def shift(values, dz=0, dy=0, dc=0):
    groups = lax.axis_size("dp")
    ny = groups // (Z_RING * CORES)
    pairs = []
    for source in range(groups):
        z, y, c = source // (ny * CORES), (source // CORES) % ny, source % CORES
        pairs.append((source, (((z + dz) % Z_RING) * ny + (y + dy) % ny) * CORES + (c + dc) % CORES))
    return lax.ppermute(values, "dp", pairs)


def swap_tensor(values, distance):
    ranks = lax.axis_size("tensor")
    return lax.ppermute(values, "tensor", [(s, s ^ distance) for s in range(ranks)])


def sum_tensor(values):
    distance = 1
    while distance < lax.axis_size("tensor"):
        values = values + swap_tensor(values, distance)
        distance *= 2
    return values


def flip_halves(values, axis):
    first, second = jnp.split(values, 2, axis=axis)
    return jnp.concatenate([second, first], axis=axis)


def by_core(core, own, other, axis):
    return jnp.where(
        core == 0, jnp.concatenate([own, other], axis=axis), jnp.concatenate([other, own], axis=axis)
    )


def half_of(values, which, axis):
    size = values.shape[axis] // CORES
    return lax.dynamic_slice_in_dim(values, which * size, size, axis)


def scale_rows_kernel(v_ref, square_ref, gain_ref, o_ref, scale_ref):
    scale = lax.rsqrt(square_ref[...] / INNER + EPSILON)
    scale_ref[...] = scale
    o_ref[...] = (v_ref[...] * scale * gain_ref[...]).astype(jnp.bfloat16)


def scale_rows(values, square, gain):
    rows, cols = values.shape
    step = 256
    wide = pl.BlockSpec((step, cols), lambda i: (i, 0))
    thin = pl.BlockSpec((step, 1), lambda i: (i, 0))
    return pl.pallas_call(
        scale_rows_kernel,
        grid=(rows // step,),
        in_specs=[wide, thin, pl.BlockSpec((1, cols), lambda i: (0, 0))],
        out_specs=[wide, thin],
        out_shape=[
            jax.ShapeDtypeStruct((rows, cols), jnp.bfloat16), jax.ShapeDtypeStruct((rows, 1), jnp.float32),
        ],
        cost_estimate=pl.CostEstimate(flops=2 * rows * cols, bytes_accessed=6 * rows * cols, transcendentals=0),
        name="scale_rows",
    )(values, square, gain)


def blank_kernel(*refs):
    pass


def blanks(*shapes):
    return pl.pallas_call(
        blank_kernel,
        out_shape=[jax.ShapeDtypeStruct(s, jnp.bfloat16) for s in shapes],
        out_specs=[pl.BlockSpec(memory_space=pl.ANY) for _ in shapes],
        name="blanks",
    )()


def gather_weight(full, weight, shared=None, halves=None, merge=1):
    z, y, core, ny = place_on()

    def columns(which):
        parts = [half_of(weight, which, 1)]
        if shared is not None:
            parts += [shared, half_of(halves, which, 1)]
            spare = -sum(p.shape[1] for p in parts) % 128
            parts.append(jnp.zeros((weight.shape[0], spare), weight.dtype))
        return jnp.concatenate(parts, axis=1)

    got = shift(columns(1 - core), dc=1)
    piece = by_core(core, columns(core), got, 0)
    rows = piece.shape[0]

    def put(full, part, dz, dy):
        at = ((z - dz) % Z_RING * ny + (y - dy) % ny) * rows
        return lax.dynamic_update_slice_in_dim(full, part, at, 0)

    ring = [piece]
    for dz in range(Z_RING - 1):
        ring.append(shift(ring[dz], dz=1))
    for send in range(Z_RING // merge):
        span = range(send * merge, (send + 1) * merge)
        both = jnp.concatenate([ring[i] for i in span], axis=0)
        for dy in range(1, ny):
            across = shift(both, dy=dy)
            for k, i in enumerate(span):
                full = put(full, across[k * rows : (k + 1) * rows], i, dy)
        for i in span:
            full = put(full, ring[i], i, 0)
    return full


def swap_rows(run, core):
    got = shift(half_of(run, 1 - core, 0).astype(jnp.bfloat16), dc=1).astype(jnp.float32)
    return half_of(run, core, 0), got


def reduce_weight(partial, sends):
    z, y, core, ny = place_on()
    rows = partial.shape[0] // (Z_RING * ny)
    f = jnp.float32

    def part(dz, dy):
        at = ((z - dz) % Z_RING * ny + (y + dy) % ny) * rows
        return lax.dynamic_slice_in_dim(partial, at, rows, 0)

    if not sends:
        def line(dz):
            return lax.dynamic_slice_in_dim(partial, (z + dz) % Z_RING * ny * rows, ny * rows, 0)

        run = line(0).astype(f)
        for dz in range(1, Z_RING):
            run = run + shift(line(dz), dz=dz).astype(f)
        total = lax.dynamic_slice_in_dim(run, y * rows, rows, 0)
        for dy in range(1, ny):
            there = lax.dynamic_slice_in_dim(run, (y + dy) % ny * rows, rows, 0)
            total = total + shift(there.astype(jnp.bfloat16), dy=dy).astype(f)
        return swap_rows(total, core)
    owns = [part(dz, 0).astype(f) for dz in range(1, Z_RING + 1)]
    for send, size in enumerate(sends):
        begin = sum(sends[:send])
        span = range(begin, begin + size)
        for dy in range(1, ny):
            across = shift(jnp.concatenate([part(i + 1, dy) for i in span], axis=0), dy=dy)
            for k, i in enumerate(span):
                owns[i] = owns[i] + across[k * rows : (k + 1) * rows].astype(f)
    run = owns[0]
    for dz in range(1, Z_RING):
        run = shift(run.astype(jnp.bfloat16), dz=1).astype(f) + owns[dz]
    return swap_rows(run, core)


def body(
    tokens, cotangent, norm_gain, w_gate, w_input, w_state, w_step, conv_weight, conv_bias,
    conv_state_weight, conv_state_bias, step_bias, decay_log, skip_gain, gate_gain, w_out,
    stats_gate, stats_input, stats_state, stats_out, roots_gate, roots_input, roots_state, roots_out,
    seq_lens, balance_perm, inverse_perm,
):
    f = jnp.float32
    groups = lax.axis_size("dp")
    tensor_ranks = lax.axis_size("tensor")
    _, _, core, ny = place_on()
    local_rows = tokens.shape[0]
    slot_rows = local_rows // groups
    group_rows = local_rows * tensor_ranks
    heads = step_bias.shape[0] // CORES
    width = w_gate.shape[1] // CORES

    tokens_f = tokens.astype(f)
    scale_in = lax.rsqrt(jnp.mean(tokens_f * tokens_f, axis=1) + EPSILON)
    gain_in = norm_gain.astype(f)
    normed = (tokens_f * scale_in[:, None] * gain_in[None, :]).astype(jnp.bfloat16)
    send_choose = rank_matrix(inverse_perm)

    edge = width + 2 * STATE
    spare = -(edge + heads) % 128
    all_gate, all_input, all_out = blanks((D, width), (D, edge + heads + spare), (D, width))
    gate_w = gather_weight(all_gate, w_gate)
    input_w = gather_weight(all_input, w_input, w_state, w_step)
    out_w = gather_weight(all_out, w_out)

    source = balance_perm // local_rows
    row_key = (source % tensor_ranks * groups + source // tensor_ranks) * group_rows + jnp.arange(
        group_rows, dtype=jnp.int32
    )
    place = rank_matrix(row_key)

    def dispatch(values):
        sent = move_rows(send_choose, values).reshape(groups, slot_rows, D)
        arrived = lax.all_to_all(sent, "dp", split_axis=0, concat_axis=0, tiled=True)
        arrived = arrived.reshape(local_rows, D)
        if tensor_ranks == 2:
            rank = lax.axis_index("tensor")
            got = swap_tensor(arrived, 1)
            both = by_core(rank, arrived, got, 0)
        else:
            both = lax.all_gather(arrived, "tensor", axis=0, tiled=True)
        own = move_back(place, both)
        partner = shift(own, dc=1)
        return jnp.concatenate([own, partner], axis=0)

    normed_bal = dispatch(normed)
    cot_bal = dispatch(cotangent)

    lens = jnp.concatenate([seq_lens, shift(seq_lens, dc=1)], axis=0)
    first = segment_info(lens[0], group_rows)
    second = segment_info(lens[1], group_rows)
    segment = jnp.concatenate([first[0], second[0]])
    position = jnp.concatenate([first[1], second[1]])

    d_normal = jnp.dot(cot_bal, out_w, preferred_element_type=f)
    gate_proj = jnp.dot(normed_bal, gate_w, preferred_element_type=f)
    joined = jnp.dot(normed_bal, input_w, preferred_element_type=f)
    step_full = jnp.dot(normed_bal, input_w[:, edge : edge + heads], preferred_element_type=f)
    step_full = step_full + half_of(step_bias, core, 0).astype(f)[None, :]
    tiles = heads // TILEH
    step_tiles = step_full.reshape(CORES * group_rows, tiles, TILEH).transpose(1, 0, 2)
    step_len = jax.nn.softplus(step_tiles)
    step_slope = jax.nn.sigmoid(step_tiles)
    consts = mixer_consts(
        half_of(conv_weight, core, 1), half_of(conv_bias, core, 0), conv_state_weight, conv_state_bias,
        half_of(skip_gain, core, 0), half_of(decay_log, core, 0), segment, position,
    )
    gain_gate = half_of(gate_gain, core, 0).astype(f)
    mixed, gated_out, square = mixer_forward(gate_proj, joined, step_len, consts, group_rows)

    def row_total(values):
        values = values + flip_halves(shift(values, dc=1), 0)
        return sum_tensor(values)

    inner_dot = row_total(jnp.sum(gated_out * gain_gate[None, :] * d_normal, axis=1))
    normal, gate_scale = scale_rows(gated_out, row_total(square[:, 0])[:, None], gain_gate[None, :])
    coef = gate_scale**3 * inner_dot[:, None] / INNER

    def give_back(own, other):
        got = shift(other, dc=1)
        own = (own.astype(f) + got.astype(f)).astype(jnp.bfloat16)
        arranged = move_rows(place, own)
        if tensor_ranks == 2:
            rank = lax.axis_index("tensor")
            mine = half_of(arranged, rank, 0).astype(f)
            got = swap_tensor(half_of(arranged, 1 - rank, 0), 1)
            total = (mine + got.astype(f)).astype(jnp.bfloat16)
        else:
            total = lax.psum_scatter(arranged, "tensor", scatter_dimension=0, tiled=True)
        returned = lax.all_to_all(total.reshape(groups, slot_rows, D), "dp", split_axis=0, concat_axis=0, tiled=True)
        return move_back(send_choose, returned.reshape(local_rows, D)).astype(f)

    branch_other = contract_cols(normal[group_rows:], out_w).astype(jnp.bfloat16)
    branch_own = contract_cols(normal[:group_rows], out_w)
    branch = give_back(branch_own, branch_other)
    out_part = contract_rows(cot_bal, normal).astype(jnp.bfloat16)
    out_own, out_got = reduce_weight(out_part, ())
    out_grad = by_core(core, out_own, out_got, 1)

    sig_gate = jax.nn.sigmoid(gate_proj)
    silu_gate = gate_proj * sig_gate
    d_gated = d_normal * gate_scale * gain_gate[None, :] - gated_out * coef
    d_gate = (d_gated * mixed * (sig_gate + silu_gate * (1.0 - sig_gate))).astype(jnp.bfloat16)
    gate_own, gate_got = reduce_weight(contract_rows(normed_bal, d_gate).astype(jnp.bfloat16), (4,))
    gate_grad = by_core(core, gate_own, gate_got, 1)

    def back_half(at):
        d_inner, d_step, d_state, rows_part, heads_part, state_part = mixer_backward(
            gate_proj, joined, mixed, d_normal, gate_scale, coef, gain_gate[None, :],
            step_len, step_slope, consts, group_rows, at,
        )
        d_step = d_step.transpose(1, 0, 2).reshape(group_rows, heads).astype(jnp.bfloat16)
        empty = jnp.zeros((group_rows, spare), jnp.bfloat16)
        return jnp.concatenate([d_inner, d_state, d_step, empty], axis=1), rows_part, heads_part, state_part

    second_half = back_half(1)
    first_half = back_half(0)
    d_joined = jnp.concatenate([first_half[0], second_half[0]], axis=0)
    row_sums, head_sums, state_sums = [one + two for one, two in zip(first_half[1:], second_half[1:])]
    joined_own, joined_got = reduce_weight(contract_rows(normed_bal, d_joined).astype(jnp.bfloat16), (1, 1, 2))
    input_grad = by_core(core, joined_own[:, :width], joined_got[:, :width], 1)
    state_grad = sum_tensor(joined_own[:, width:edge] + joined_got[:, width:edge])
    step_grad = by_core(core, joined_own[:, edge : edge + heads], joined_got[:, edge : edge + heads], 1)

    def column_term(at):
        part = slice(at * group_rows, (at + 1) * group_rows)
        half = (first_half, second_half)[at][0]
        return contract_cols(d_gate[part], gate_w) + contract_cols(half, input_w)

    term_other = column_term(1)
    term_own = column_term(0)
    norm_gain_part = (
        jnp.sum(term_own * normed_bal[:group_rows].astype(f), axis=0)
        + jnp.sum(term_other * normed_bal[group_rows:].astype(f), axis=0)
    ) / gain_in
    d_tokens_normed = give_back(term_own, term_other.astype(jnp.bfloat16))

    head_sums = head_sums.transpose(1, 0, 2).reshape(2, heads)
    skip_sums = jnp.sum(row_sums[KCONV + 2].reshape(heads, HEADW), axis=1)
    state_sums = state_sums[: KCONV + 1]
    lanes = (KCONV + 2) * width
    split_part = jnp.concatenate([row_sums[: KCONV + 2].reshape(-1), head_sums.reshape(-1), skip_sums])
    shared_part = jnp.concatenate([norm_gain_part, state_sums.reshape(-1)])
    split_at = split_part.shape[0]
    partner = shift(jnp.concatenate([split_part, shared_part]), dc=1)
    shared_part = sum_tensor(shared_part + partner[split_at:])
    wide_part = by_core(
        core, split_part[:lanes].reshape(KCONV + 2, width), partner[:lanes].reshape(KCONV + 2, width), 1
    )
    thin_part = by_core(core, split_part[lanes:].reshape(3, heads), partner[lanes:split_at].reshape(3, heads), 1)
    packed = jnp.concatenate([wide_part.reshape(-1), thin_part.reshape(-1), shared_part])
    packed_low = packed.astype(jnp.bfloat16)
    for dz in range(Z_RING):
        for dy in range(ny):
            if (dz, dy) != (0, 0):
                packed = packed + shift(packed_low, dz=dz, dy=dy).astype(f)
    lanes, split_at = CORES * lanes, CORES * split_at
    wide_sums = packed[:lanes].reshape(KCONV + 2, CORES * width)
    thin_sums = packed[lanes:split_at].reshape(3, CORES * heads)
    shared = packed[split_at:]
    norm_gain_grad = shared[:D]
    conv_state_grads = shared[D:].reshape(KCONV + 1, 2 * STATE)

    block_out = tokens_f + branch
    dot_in = jnp.sum(tokens_f * gain_in[None, :] * d_tokens_normed, axis=1)
    tokens_grad = (
        cotangent.astype(f)
        + d_tokens_normed * scale_in[:, None] * gain_in[None, :]
        - tokens_f * (scale_in**3 * dot_in / D)[:, None]
    )
    new_gate = shampoo(w_gate, gate_grad, stats_gate, roots_gate)
    new_input = shampoo(w_input, input_grad, stats_input, roots_input)
    new_state = shampoo(w_state, state_grad, stats_state, roots_state)
    new_out = shampoo(w_out, out_grad, stats_out, roots_out)
    return (
        block_out, tokens_grad, norm_gain_grad, gate_grad, input_grad, state_grad, step_grad,
        wide_sums[:KCONV], wide_sums[KCONV], conv_state_grads[:KCONV], conv_state_grads[KCONV],
        thin_sums[0], thin_sums[1], thin_sums[2], wide_sums[KCONV + 1], out_grad,
        new_gate[0], new_input[0], new_state[0], new_out[0],
        new_gate[1], new_input[1], new_state[1], new_out[1],
        new_gate[2], new_input[2], new_state[2], new_out[2],
    )


def solution(mesh):
    placed = (
        P(("dp", "tensor"), None),
        P(("dp", "tensor"), None),
        P(),
        P("dp", "tensor"),
        P("dp", "tensor"),
        P("dp", None),
        P("dp", "tensor"),
        P(None, "tensor"),
        P("tensor"),
        P(),
        P(),
        P("tensor"),
        P("tensor"),
        P("tensor"),
        P("tensor"),
        P("dp", "tensor"),
        P("dp", "tensor", None, None, None),
        P("dp", "tensor", None, None, None),
        P("dp", None, None, None, None),
        P("dp", "tensor", None, None, None),
        P("dp", "tensor", None, None, None),
        P("dp", "tensor", None, None, None),
        P("dp", None, None, None, None),
        P("dp", "tensor", None, None, None),
        P("dp", None),
        P("dp"),
        P(("dp", "tensor")),
    )
    return jax.shard_map(
        body,
        mesh=mesh,
        in_specs=placed,
        out_specs=(
            P(("dp", "tensor"), None),
            P(("dp", "tensor"), None),
            P(),
            P("dp", "tensor"),
            P("dp", "tensor"),
            P("dp", None),
            P("dp", "tensor"),
            P(None, "tensor"),
            P("tensor"),
            P(),
            P(),
            P("tensor"),
            P("tensor"),
            P("tensor"),
            P("tensor"),
            P("dp", "tensor"),
            P("dp", "tensor", None, None, None),
            P("dp", "tensor", None, None, None),
            P("dp", None, None, None, None),
            P("dp", "tensor", None, None, None),
            P("dp", "tensor"),
            P("dp", "tensor"),
            P("dp", None),
            P("dp", "tensor"),
            P("dp", "tensor"),
            P("dp", "tensor"),
            P("dp", None),
            P("dp", "tensor"),
        ),
        check_vma=False,
    )
```
